256 devices in a mesh: groups: 2 (over z), rows: 16 (over y, core), cols: 8 (over x).
Axes of the slice: x: 8, y: 8, z: 2, core: 2. Of those that a mesh axis runs over, the one named last changes fastest.
The devices are a block of a 8x8x16 slice.
Arguments:
- pair_state: float32 [768, 384, 128], P(('groups', 'rows'), 'cols'), parts along dimension 0, may hold values from -6 to 6
- token_mask: int32 [768], P('groups'), parts along dimension 0, may hold values 0 or 1
- norm_gain: float32 [2, 128], replicated, may hold values from 0.25 to 1.75
- norm_bias: float32 [2, 128], replicated, may hold values from -3 to 3
- proj_weight: float32 [2, 128, 512], replicated, may hold values from -0.5 to 0.5
- gate_weight: float32 [2, 128, 128], replicated, may hold values from -0.5 to 0.5
- out_gain: float32 [2, 128], replicated, may hold values from 0.25 to 1.75
- out_bias: float32 [2, 128], replicated, may hold values from -3 to 3
- out_weight: float32 [2, 128, 128], replicated, may hold values from -0.5 to 0.5
Outputs:
- pair_out: float32 [768, 384, 128], P(('groups', 'rows'), 'cols'), parts along dimension 0
The draws below stay inside these ranges and needn't reach their ends.
There are 2 independent parts, one for each index of `groups`. The reference program is written for one: setup_inputs(seed, part) draws one part's arguments, and reference() takes and returns one part's arrays. A program takes and returns all parts, laid end to end along the dimension named above; an argument that names none is the same for every part. Nothing has to cross between parts.
All inputs are finite; a program needn't handle non-finite values.
Results may differ from the reference program's by a relative error of at most 0.0001.
Values sent between devices are 32-bit elements; how exact they have to be, the bound alone decides.
A program may use at most 128 MiB of HBM per device.

```python
import jax
import jax.numpy as jnp
from jax import lax

C = 128
H = 128
N = 384


def plant(array, rng, least, high):
    shape = array.shape
    place = [jax.random.randint(jax.random.fold_in(rng, axis), (), 0, shape[axis]) for axis in range(len(shape))]
    array = array.at[tuple(place)].set(least)
    longest = shape.index(max(shape))
    place[longest] = (place[longest] + 1) % shape[longest]
    return array.at[tuple(place)].set(high)


def block_scale(stream_key, extent, pieces, smallest, top_value):
    def one(axis_at, shards_of):
        draws = jax.random.uniform(jax.random.fold_in(jax.random.fold_in(stream_key, 6), axis_at), (shards_of,), jnp.float32, smallest / len(pieces), top_value / len(pieces))
        return jnp.repeat(jnp.exp(draws), extent[axis_at] // shards_of).reshape((-1,) + (1,) * (len(extent) - axis_at - 1))

    level = one(*pieces[0])
    for cut in pieces[1:]:
        level = level * one(*cut)
    return level


def scatter_about(rng, shape, scale, limit, cuts=(), dtype=jnp.bfloat16):
    level = block_scale(rng, shape, cuts, -0.22, 0.18) if cuts else 1.0
    values = jax.random.normal(rng, shape, jnp.float32) * scale * level
    return jnp.minimum(jnp.maximum(values, -limit), limit).astype(dtype)


def setup_inputs(seed: int = 0, part: int = 0) -> dict:
    streams_of = jax.random.split(jax.random.key(seed), 10)
    part_keys = jax.random.split(jax.random.fold_in(streams_of[9], part), 10)
    return {
        "pair_state": scatter_about(part_keys[0], (N, N, C), 1.0, 6.0, ((0, 16), (1, 8)), jnp.float32),
        "token_mask": plant((jax.random.randint(part_keys[1], (N,), 0, 4) < 3).astype(jnp.int32), jax.random.fold_in(part_keys[1], 1), 0, 1),
        "norm_gain": jnp.clip(1.0 + 0.15 * jax.random.normal(streams_of[2], (2, C), jnp.float32), 0.25, 1.75),
        "norm_bias": scatter_about(streams_of[3], (2, C), 0.5, 3.0, (), jnp.float32),
        "proj_weight": scatter_about(streams_of[4], (2, C, 4 * H), C ** -0.5, 0.5, (), jnp.float32),
        "gate_weight": scatter_about(streams_of[5], (2, C, C), C ** -0.5, 0.5, (), jnp.float32),
        "out_gain": jnp.clip(1.0 + 0.15 * jax.random.normal(streams_of[6], (2, H), jnp.float32), 0.25, 1.75),
        "out_bias": scatter_about(streams_of[7], (2, H), 0.5, 3.0, (), jnp.float32),
        "out_weight": scatter_about(streams_of[8], (2, H, C), H ** -0.5, 0.5, (), jnp.float32),
    }


eps = 1e-05

def normalize(values, gain, shift):
    center = values - lax.optimization_barrier(jnp.mean(values, axis=-1, keepdims=True))
    spread = lax.optimization_barrier(jnp.mean(center * center, axis=-1, keepdims=True))
    return center * lax.rsqrt(spread + eps) * gain + shift

def update_once(state, pair_mask, segment, norm_gain, norm_bias, proj_weight, gate_weight, out_gain, out_bias, out_weight):
    width = proj_weight.shape[2] // 4
    normed = normalize(state, norm_gain[segment], norm_bias[segment])
    hidden = jnp.einsum('ijc,cf->ijf', normed, proj_weight[segment], precision=lax.Precision.HIGHEST)
    left_side = pair_mask[:, :, None] * jax.nn.sigmoid(hidden[:, :, :width]) * hidden[:, :, width:2 * width]
    right_side = pair_mask[:, :, None] * jax.nn.sigmoid(hidden[:, :, 2 * width:3 * width]) * hidden[:, :, 3 * width:]
    gating = jax.nn.sigmoid(jnp.einsum('ijc,cd->ijd', normed, gate_weight[segment], precision=lax.Precision.HIGHEST))
    if segment == 0:
        mixed = jnp.einsum('ikh,jkh->ijh', left_side, right_side, precision=lax.Precision.HIGHEST)
    else:
        mixed = jnp.einsum('kih,kjh->ijh', left_side, right_side, precision=lax.Precision.HIGHEST)
    result = jnp.einsum('ijh,hc->ijc', normalize(mixed, out_gain[segment], out_bias[segment]), out_weight[segment], precision=lax.Precision.HIGHEST)
    return state + gating * result

def reference(pair_state, token_mask, norm_gain, norm_bias, proj_weight, gate_weight, out_gain, out_bias, out_weight):
    maskf = token_mask.astype(jnp.float32)
    pair_mask = maskf[:, None] * maskf[None, :]
    state = pair_state
    for segment in range(2):
        state = update_once(state, pair_mask, segment, norm_gain, norm_bias, proj_weight, gate_weight, out_gain, out_bias, out_weight)
    return state
```

```python
import functools

import jax
import jax.numpy as jnp
from jax import lax
from jax.experimental import pallas as pl
from jax.experimental.pallas import tpu as pltpu
from jax.sharding import PartitionSpec as P

MESH = pl.DeviceIdType.MESH
eps = 1e-05
LANES = 128
SUB = 8
F32 = jnp.float32
BF16 = jnp.bfloat16


def high_low(values):
    high = values.astype(BF16)
    low = (values - high.astype(F32)).astype(BF16)
    return high, low


def columns_of(row):
    return jnp.broadcast_to(row, (LANES, LANES)).T


def block_transpose(parts, width):
    count, tiles = len(parts), len(parts[0])
    lane = lax.broadcasted_iota(jnp.int32, (SUB, LANES), 1)
    rolled = {}

    def turned(a, u, shift):
        key = (a, u, shift)
        if key not in rolled:
            rolled[key] = parts[a][u] if shift == 0 else pltpu.roll(parts[a][u], shift, 1)
        return rolled[key]

    out = []
    for b in range(count):
        row = []
        for t in range(tiles):
            acc = None
            at, end = t * LANES, (t + 1) * LANES
            while at < end:
                a = at // width
                source = b * width + at - a * width
                u = source // LANES
                stop = min(end, (a + 1) * width, at + (u + 1) * LANES - source)
                piece = turned(a, u, (at - source) % LANES)
                acc = piece if acc is None else jnp.where(lane >= at - t * LANES, piece, acc)
                at = stop
            row.append(acc)
        out.append(row)
    return out


def kernel(
    sizes,
    x_hbm,
    mask_hbm,
    norm_gain_hbm,
    norm_bias_hbm,
    proj_hbm,
    gate_hbm,
    out_gain_hbm,
    out_bias_hbm,
    out_hbm,
    y_ref,
    x_in,
    mask_in,
    norm_gain_in,
    norm_bias_in,
    proj_in,
    gate_in,
    out_gain_in,
    out_bias_in,
    out_in,
    weights,
    columns,
    mask_rows,
    mask_chunk,
    state,
    gating,
    normed,
    send_right,
    have_right,
    send_left,
    have_left,
    send_mixed,
    have_mixed,
    send_both,
    have_both,
    send_next,
    have_next,
    right_rows,
    right_cat,
    chunk_a,
    chunk_b,
    total,
    load_sem,
    send_sem,
    recv_sem,
):
    nr, nc, ri, cj = sizes
    slots = nr * nc
    rows_per = ri * cj // LANES
    chunks = ri // SUB
    per = rows_per // chunks
    tiles = nr * ri // LANES
    half = nr // SUB
    chunk_pos = per * LANES

    r, c = lax.axis_index("rows"), lax.axis_index("cols")
    me = c * nr + r
    pair, core = r // 2, lax.rem(r, 2)
    pairs = nr // 2
    cols = [lax.rem(c + d, nc) for d in range(nc)]
    cores = [core, 1 - core]
    order = [d for d in (4, 1, 7, 2, 6, 3, 5, 0) if d < nc]

    loads = [
        pltpu.make_async_copy(src, dst, load_sem.at[i])
        for i, (src, dst) in enumerate(
            (
                (x_hbm, x_in),
                (norm_gain_hbm, norm_gain_in),
                (norm_bias_hbm, norm_bias_in),
                (proj_hbm, proj_in),
                (mask_hbm, mask_in),
                (gate_hbm, gate_in),
                (out_gain_hbm, out_gain_in),
                (out_bias_hbm, out_bias_in),
                (out_hbm, out_in),
            )
        )
    ]
    for load in loads:
        load.start()

    def to_all(act):
        def step(i, carry):
            turned = []
            for d in range(pairs):
                far = lax.rem(i + d, pairs)
                turned.append((far, lax.rem(pair + far, pairs) * 2))
            for dx in order:
                for k in range(2):
                    far, base = turned[(dx + 4 * k) % pairs]
                    row = base + cores[k]

                    def go(row=row, dx=dx):
                        act(cols[dx] * nr + row, {"rows": row, "cols": cols[dx]})

                    if dx == 0 and k == 0:
                        pl.when(far != 0)(go)
                    else:
                        go()
            return carry

        lax.fori_loop(0, pairs, step, 0)

    barrier = pltpu.get_barrier_semaphore()
    to_all(lambda slot, device: pl.semaphore_signal(barrier, inc=1, device_id=device, device_id_type=MESH))

    def send(src, dst, stride, base, count, sem):
        def act(slot, device):
            pltpu.make_async_remote_copy(
                src_ref=src.at[pl.ds(slot * stride + base, count)],
                dst_ref=dst.at[pl.ds(me * stride + base, count)],
                send_sem=send_sem.at[sem],
                recv_sem=recv_sem.at[sem],
                device_id=device,
                device_id_type=MESH,
            ).start()

        to_all(act)
        for q in range(count):
            dst[pl.ds(me * stride + base + q, 1), :] = src[pl.ds(me * stride + base + q, 1), :]

    def await_bytes(buffer, count, sems, sem):
        span = buffer.at[pl.ds(0, (slots - 1) * count)]
        pltpu.make_async_copy(span, span, sems.at[sem]).wait()

    def prepare_weights(u):
        def one(values, at):
            high, low = high_low(values.T)
            rows = pl.ds(at * LANES, LANES)
            weights[u, rows, 0:LANES] = high
            weights[u, rows, LANES : 2 * LANES] = low
            weights[u, rows, 2 * LANES : 3 * LANES] = high

        for f in range(4):
            one(proj_in[u, :, f * LANES : (f + 1) * LANES], f)
        one(gate_in[u], 4)
        one(out_in[u], 5)

    def prepare_columns(u):
        for i, ref in enumerate((norm_gain_in, norm_bias_in, out_gain_in, out_bias_in)):
            columns[4 * u + i] = columns_of(ref[pl.ds(u, 1), :])

    def normalize(values, gain, bias):
        center = values - jnp.mean(values, axis=0, keepdims=True)
        spread = jnp.mean(center * center, axis=0, keepdims=True)
        return center * lax.rsqrt(spread + eps) * gain + bias

    def normalize_into(values, u, lanes, first):
        high, low = high_low(normalize(values, columns[4 * u + first], columns[4 * u + first + 1]))
        normed[0:LANES, lanes] = high
        normed[LANES : 2 * LANES, lanes] = high
        normed[2 * LANES : 3 * LANES, lanes] = low

    def product(u, first, count, lanes):
        return jnp.dot(
            weights[u, first * LANES : (first + count) * LANES, :],
            normed[:, lanes],
            preferred_element_type=F32,
        )

    def side(u, first, lanes, buffer, stride, base):
        hidden = product(u, first, 2, lanes)
        values = jax.nn.sigmoid(hidden[0:LANES]) * hidden[LANES:]
        for b in range(slots // SUB):
            for t in range(per):
                buffer[pl.ds(b * SUB * stride + base + t, SUB, stride=stride), :] = values[
                    b * SUB : (b + 1) * SUB, t * LANES : (t + 1) * LANES
                ]

    def chunk_lanes(k):
        return slice(k * chunk_pos, (k + 1) * chunk_pos)

    def gather_block(buffer, stride, base, b8):
        parts = [
            [
                buffer[pl.ds((a * nr + b8 * SUB) * stride + base + t, SUB, stride=stride), :]
                for t in range(per)
            ]
            for a in range(nc)
        ]
        return block_transpose(parts, cj)

    def scatter_block(parts, buffer, stride, base, b8):
        for a, row in enumerate(block_transpose(parts, cj)):
            for t in range(per):
                buffer[pl.ds((a * nr + b8 * SUB) * stride + base + t, SUB, stride=stride), :] = row[t]

    def finish(u, k, have):
        for t in range(per):
            q = k * per + t
            lanes = slice(q * LANES, (q + 1) * LANES)
            mixed = jnp.concatenate(
                [have[pl.ds(b * SUB * rows_per + q, SUB, stride=rows_per), :] for b in range(slots // SUB)], axis=0
            )
            normalize_into(mixed, u, lanes, 2)
        lanes = chunk_lanes(k)
        return state[:, lanes] + gating[:, lanes] * product(u, 5, 1, lanes)

    loads[0].wait()
    loads[1].wait()
    loads[2].wait()
    loads[3].wait()
    for load in loads[4:]:
        load.wait()
    prepare_weights(0)
    prepare_columns(0)
    for q in range(rows_per):
        lanes = slice(q * LANES, (q + 1) * LANES)
        values = x_in[q * LANES : (q + 1) * LANES, :].T
        state[:, lanes] = values
        normalize_into(values, 0, lanes, 0)
    for k in range(chunks):
        side(0, 2, chunk_lanes(k), send_right, rows_per, k * per)
    pl.semaphore_wait(barrier, slots - 1)
    send(send_right, have_right, rows_per, 0, rows_per, 0)
    for k in range(chunks):
        side(0, 0, chunk_lanes(k), send_left, rows_per, k * per)
        send(send_left, have_left, rows_per, k * per, per, 1 + k)
    for k in range(chunks):
        gating[:, chunk_lanes(k)] = jax.nn.sigmoid(product(0, 4, 1, chunk_lanes(k)))
    prepare_weights(1)
    prepare_columns(1)
    mask = mask_in[...].astype(F32)
    for t in range(tiles):
        mask_rows[t * LANES : (t + 1) * LANES, :] = columns_of(mask[t : t + 1, :])
    for k in range(chunks):
        for b in range(SUB):
            for b8 in range(half):
                mask_chunk[k, pl.ds(b * nr + b8 * SUB, SUB), :] = mask_rows[
                    pl.ds(b8 * SUB * ri + k * SUB + b, SUB, stride=ri), :
                ]

    await_bytes(have_right, rows_per, recv_sem, 0)
    for k in range(chunks):
        for b8 in range(half):
            for b, row in enumerate(gather_block(have_right, rows_per, k * per, b8)):
                for t in range(tiles):
                    right_rows[pl.ds(t * nr * ri + b8 * SUB * ri + k * SUB + b, SUB, stride=ri), :] = row[t]
    tokens = nr * ri
    for t in range(tiles):
        high, low = high_low(right_rows[t * tokens : (t + 1) * tokens, :] * mask_rows[...])
        right_cat[:, t * LANES : (t + 1) * LANES] = high
        right_cat[:, tokens + t * LANES : tokens + (t + 1) * LANES] = high
        right_cat[:, 2 * tokens + t * LANES : 2 * tokens + (t + 1) * LANES] = low
    for k in range(chunks):
        await_bytes(have_left, per, recv_sem, 1 + k)
        for b8 in range(half):
            for b, row in enumerate(gather_block(have_left, rows_per, k * per, b8)):
                for t in range(tiles):
                    chunk_a[pl.ds(b * nr + b8 * SUB, SUB), t * LANES : (t + 1) * LANES] = (
                        row[t] * mask[t : t + 1, :] * mask_chunk[k, pl.ds(b * nr + b8 * SUB, SUB), :]
                    )
        high, low = high_low(chunk_a[...])
        chunk_b[...] = lax.dot_general(
            jnp.concatenate([high, low, high], axis=1),
            right_cat[...],
            (((1,), (1,)), ((), ())),
            preferred_element_type=F32,
        )
        for b8 in range(half):
            parts = [
                [chunk_b[pl.ds(b * nr + b8 * SUB, SUB), t * LANES : (t + 1) * LANES] for t in range(tiles)]
                for b in range(SUB)
            ]
            scatter_block(parts, send_mixed, rows_per, k * per, b8)
        send(send_mixed, have_mixed, rows_per, k * per, per, 4 + k)

    for k in range(chunks):
        await_bytes(have_mixed, per, recv_sem, 4 + k)
        lanes = chunk_lanes(k)
        state[:, lanes] = finish(0, k, have_mixed)
        for t in range(per):
            q = k * per + t
            tile = slice(q * LANES, (q + 1) * LANES)
            normalize_into(state[:, tile], 1, tile, 0)
        side(1, 0, lanes, send_both, 2 * rows_per, 2 * per * k)
        side(1, 2, lanes, send_both, 2 * rows_per, 2 * per * k + per)
        send(send_both, have_both, 2 * rows_per, 2 * per * k, 2 * per, 7 + k)
        gating[:, lanes] = jax.nn.sigmoid(product(1, 4, 1, lanes))

    for k in range(chunks):
        await_bytes(have_both, 2 * per, recv_sem, 7 + k)
        for b8 in range(half):
            for b, row in enumerate(gather_block(have_both, 2 * rows_per, 2 * per * k, b8)):
                for t in range(tiles):
                    chunk_a[pl.ds(b * nr + b8 * SUB, SUB), t * LANES : (t + 1) * LANES] = row[t] * mask[t : t + 1, :]
            for b, row in enumerate(gather_block(have_both, 2 * rows_per, 2 * per * k + per, b8)):
                for t in range(tiles):
                    chunk_b[pl.ds(b * nr + b8 * SUB, SUB), t * LANES : (t + 1) * LANES] = (
                        row[t] * mask[t : t + 1, :] * mask_chunk[k, pl.ds(b * nr + b8 * SUB, SUB), :]
                    )
        left_t = jnp.concatenate(
            [chunk_a[:, t * LANES : (t + 1) * LANES].T for t in range(tiles)], axis=0
        )
        high, low = high_low(left_t)
        right_high, right_low = high_low(chunk_b[...])
        part = jnp.dot(
            jnp.concatenate([high, low, high], axis=1),
            jnp.concatenate([right_high, right_high, right_low], axis=0),
            preferred_element_type=F32,
        )
        for t in range(tiles):
            rows = slice(t * tokens, (t + 1) * tokens)
            if k == 0:
                total[rows, :] = part[:, t * LANES : (t + 1) * LANES]
            else:
                total[rows, :] += part[:, t * LANES : (t + 1) * LANES]
    for k in range(chunks):
        for b8 in range(half):
            parts = [
                [
                    total[pl.ds(t * tokens + b8 * SUB * ri + k * SUB + b, SUB, stride=ri), :]
                    for t in range(tiles)
                ]
                for b in range(SUB)
            ]
            scatter_block(parts, send_next, rows_per, k * per, b8)
        send(send_next, have_next, rows_per, k * per, per, 10 + k)
    for k in range(chunks):
        await_bytes(have_next, per, recv_sem, 10 + k)
        values = finish(1, k, have_next)
        for t in range(per):
            q = k * per + t
            y_ref[q * LANES : (q + 1) * LANES, :] = values[:, t * LANES : (t + 1) * LANES].T

    await_bytes(send_right, rows_per, send_sem, 0)
    for k in range(chunks):
        await_bytes(send_left, per, send_sem, 1 + k)
        await_bytes(send_mixed, per, send_sem, 4 + k)
        await_bytes(send_both, 2 * per, send_sem, 7 + k)
        await_bytes(send_next, per, send_sem, 10 + k)


def body(
    nr,
    nc,
    pair_state,
    token_mask,
    norm_gain,
    norm_bias,
    proj_weight,
    gate_weight,
    out_gain,
    out_bias,
    out_weight,
):
    ri, cj, channels = pair_state.shape
    hidden = proj_weight.shape[2] // 4
    tokens = token_mask.shape[0]
    slots = nr * nc
    positions = ri * cj
    assert slots == hidden == channels == LANES
    assert nr % SUB == 0 and ri % SUB == 0 and tokens == nr * ri == nc * cj and tokens % LANES == 0
    assert nc == SUB and SUB * cj == tokens and positions % LANES == 0
    rows_per = positions // LANES
    chunks = ri // SUB
    message = pltpu.VMEM((slots * rows_per, LANES), F32)
    double = pltpu.VMEM((slots * 2 * rows_per, LANES), F32)
    inputs = (
        pair_state.reshape(positions, channels),
        token_mask.reshape(tokens // LANES, LANES),
        norm_gain,
        norm_bias,
        proj_weight,
        gate_weight,
        out_gain,
        out_bias,
        out_weight,
    )
    result = pl.pallas_call(
        functools.partial(kernel, (nr, nc, ri, cj)),
        out_shape=jax.ShapeDtypeStruct((positions, channels), F32),
        in_specs=[pl.BlockSpec(memory_space=pl.ANY)] * len(inputs),
        out_specs=pl.BlockSpec(memory_space=pltpu.VMEM),
        scratch_shapes=[
            *(pltpu.VMEM(i.shape, i.dtype) for i in inputs),
            pltpu.VMEM((2, 6 * LANES, 3 * LANES), BF16),
            pltpu.VMEM((8, LANES, LANES), F32),
            pltpu.VMEM((tokens, LANES), F32),
            pltpu.VMEM((chunks, SUB * nr, LANES), F32),
            pltpu.VMEM((channels, positions), F32),
            pltpu.VMEM((channels, positions), F32),
            pltpu.VMEM((3 * LANES, positions), BF16),
            message,
            message,
            message,
            message,
            message,
            message,
            double,
            double,
            message,
            message,
            pltpu.VMEM((tokens // LANES * tokens, LANES), F32),
            pltpu.VMEM((tokens, 3 * tokens), BF16),
            pltpu.VMEM((SUB * nr, tokens), F32),
            pltpu.VMEM((SUB * nr, tokens), F32),
            pltpu.VMEM((tokens // LANES * tokens, LANES), F32),
            pltpu.SemaphoreType.DMA((len(inputs),)),
            pltpu.SemaphoreType.DMA((1 + 4 * chunks,)),
            pltpu.SemaphoreType.DMA((1 + 4 * chunks,)),
        ],
        compiler_params=pltpu.CompilerParams(
            collective_id=0, has_side_effects=True, vmem_limit_bytes=48 * 2**20
        ),
        name="triangles",
    )(*inputs)
    return result.reshape(pair_state.shape)


def solution(mesh):
    placed = (P(("groups", "rows"), "cols", None), P("groups"), P(), P(), P(), P(), P(), P(), P())
    return jax.shard_map(
        functools.partial(body, mesh.shape["rows"], mesh.shape["cols"]),
        mesh=mesh,
        in_specs=placed,
        out_specs=P(("groups", "rows"), "cols", None),
        check_vma=False,
    )
```

```python
import functools

import jax
import jax.numpy as jnp
from jax import lax
from jax.experimental import pallas as pl
from jax.experimental.pallas import tpu as pltpu
from jax.sharding import PartitionSpec as P

MESH = pl.DeviceIdType.MESH
eps = 1e-05
LANES = 128
SUB = 8
F32 = jnp.float32
BF16 = jnp.bfloat16


def high_low(values):
    high = values.astype(BF16)
    low = (values - high.astype(F32)).astype(BF16)
    return high, low


def columns_of(row):
    return jnp.broadcast_to(row, (LANES, LANES)).T


def swap_blocks(parts):
    width = LANES // SUB
    block = lax.broadcasted_iota(jnp.int32, (SUB, LANES), 1) // width
    parts = list(parts)
    for step in (1, 2, 4):
        odd = (block // step) % 2 == 1
        for a in range(SUB):
            if (a // step) % 2 == 0:
                low, high = parts[a], parts[a + step]
                parts[a] = jnp.where(odd, pltpu.roll(high, step * width, 1), low)
                parts[a + step] = jnp.where(odd, high, pltpu.roll(low, LANES - step * width, 1))
    return parts


def kernel(
    sizes,
    x_hbm,
    mask_hbm,
    norm_gain_hbm,
    norm_bias_hbm,
    proj_hbm,
    gate_hbm,
    out_gain_hbm,
    out_bias_hbm,
    out_hbm,
    y_ref,
    x_in,
    mask_in,
    norm_gain_in,
    norm_bias_in,
    proj_in,
    gate_in,
    out_gain_in,
    out_bias_in,
    out_in,
    weights,
    columns,
    mask_rows,
    mask_lanes,
    mask_near,
    mask_far,
    state,
    gating,
    normed,
    send_first,
    have_first,
    send_mixed,
    have_mixed,
    send_second,
    have_second,
    send_next,
    have_next,
    rows_a,
    rows_b,
    left_cat,
    right_cat,
    under_cat,
    blocks,
    load_sem,
    send_sem,
    recv_sem,
):
    nr, nc, ri, cj = sizes
    slots = nr * nc
    groups = ri // SUB
    half = nr // SUB
    tokens = nr * ri
    span = SUB * nr
    last = groups - 1
    early = [(a, b) for a in range(last) for b in range(last)]
    order = early + [(last, b) for b in range(last)] + [(a, last) for a in range(groups)]
    count = len(order)
    cut_a, cut_b = len(early), len(early) + last
    place = {ab: p for p, ab in enumerate(order)}

    r, c = lax.axis_index("rows"), lax.axis_index("cols")
    me = c * nr + r
    pair, core = r // 2, lax.rem(r, 2)
    pairs = nr // 2
    cols = [lax.rem(c + d, nc) for d in range(nc)]
    cores = [core, 1 - core]
    rows_at = [lax.rem(pair + d, pairs) * 2 for d in range(pairs)]
    turns = [d for d in (4, 1, 7, 2, 6, 3, 5, 0) if d < nc]

    loads = [
        pltpu.make_async_copy(src, dst, load_sem.at[i])
        for i, (src, dst) in enumerate(
            (
                (x_hbm, x_in),
                (norm_gain_hbm, norm_gain_in),
                (norm_bias_hbm, norm_bias_in),
                (proj_hbm, proj_in),
                (mask_hbm, mask_in),
                (gate_hbm, gate_in),
                (out_gain_hbm, out_gain_in),
                (out_bias_hbm, out_bias_in),
                (out_hbm, out_in),
            )
        )
    ]
    for load in loads:
        load.start()

    def to_all(act):
        def step(i, carry):
            turn, odd = i // 2, lax.rem(i, 2)
            away = pairs // 2 + turn - odd * (2 * turn + 1)
            far_row = lax.rem(pair + away, pairs) * 2
            far_col = lax.rem(c + away, nc)
            for d in turns:
                for k in range(2):
                    row, col = (far_row + cores[0], cols[d]) if k == 0 else (rows_at[d] + cores[1], far_col)

                    def go(row=row, col=col):
                        act(col * nr + row, {"rows": row, "cols": col})

                    if d == 0 and k == 0:
                        pl.when(away != 0)(go)
                    else:
                        go()
            return carry

        lax.fori_loop(0, pairs, step, 0)

    barrier = pltpu.get_barrier_semaphore()
    to_all(lambda slot, device: pl.semaphore_signal(barrier, inc=1, device_id=device, device_id_type=MESH))

    def send(src, dst, stride, base, rows, sem):
        def act(slot, device):
            pltpu.make_async_remote_copy(
                src_ref=src.at[pl.ds(slot * stride + base, rows)],
                dst_ref=dst.at[pl.ds(me * stride + base, rows)],
                send_sem=send_sem.at[sem],
                recv_sem=recv_sem.at[sem],
                device_id=device,
                device_id_type=MESH,
            ).start()

        to_all(act)
        for q in range(rows):
            dst[pl.ds(me * stride + base + q, 1), :] = src[pl.ds(me * stride + base + q, 1), :]

    def await_bytes(buffer, rows, sems, sem):
        whole = buffer.at[pl.ds(0, (slots - 1) * rows)]
        pltpu.make_async_copy(whole, whole, sems.at[sem]).wait()

    def prepare_weights(u):
        def one(values, at):
            high, low = high_low(values.T)
            rows = pl.ds(at * LANES, LANES)
            weights[u, rows, 0:LANES] = high
            weights[u, rows, LANES : 2 * LANES] = low
            weights[u, rows, 2 * LANES : 3 * LANES] = high

        for f in range(4):
            one(proj_in[u, :, f * LANES : (f + 1) * LANES], f)
        one(gate_in[u], 4)
        one(out_in[u], 5)

    def prepare_columns(u):
        for i, ref in enumerate((norm_gain_in, norm_bias_in, out_gain_in, out_bias_in)):
            columns[4 * u + i] = columns_of(ref[pl.ds(u, 1), :])

    def lanes_of(first, number=1):
        return slice(first * LANES, (first + number) * LANES)

    def normalize(values, gain, bias):
        center = values - jnp.mean(values, axis=0, keepdims=True)
        spread = jnp.mean(center * center, axis=0, keepdims=True)
        return center * lax.rsqrt(spread + eps) * gain + bias

    def normalize_into(values, u, at, first):
        high, low = high_low(normalize(values, columns[4 * u + first], columns[4 * u + first + 1]))
        normed[0:LANES, lanes_of(at)] = high
        normed[LANES : 2 * LANES, lanes_of(at)] = high
        normed[2 * LANES : 3 * LANES, lanes_of(at)] = low

    def product(u, first, number, at, tiles):
        return jnp.dot(
            weights[u, first * LANES : (first + number) * LANES, :],
            normed[:, lanes_of(at, tiles)],
            preferred_element_type=F32,
        )

    def side(u, first, at, tiles, buffer, stride, base):
        hidden = product(u, first, 2, at, tiles)
        values = jax.nn.sigmoid(hidden[0:LANES]) * hidden[LANES:]
        for b in range(slots // SUB):
            for t in range(tiles):
                buffer[pl.ds(b * SUB * stride + base + t, SUB, stride=stride), :] = values[
                    b * SUB : (b + 1) * SUB, lanes_of(t)
                ]

    def at_owner(buffer, stride, row, b8):
        return swap_blocks(
            [buffer[pl.ds((a * nr + b8 * SUB) * stride + row, SUB, stride=stride), :] for a in range(nc)]
        )

    def to_owners(parts, buffer, stride, row, b8):
        for a, part in enumerate(swap_blocks(parts)):
            buffer[pl.ds((a * nr + b8 * SUB) * stride + row, SUB, stride=stride), :] = part

    def finish(u, first, number, have):
        for t in range(number):
            normalize_into(
                jnp.concatenate(
                    [have[pl.ds(b * SUB * count + first + t, SUB, stride=count), :] for b in range(slots // SUB)],
                    axis=0,
                ),
                u,
                t,
                2,
            )
        lanes = lanes_of(first, number)
        return state[:, lanes] + gating[:, lanes] * product(u, 5, 1, 0, number)

    def pieces(p):
        a, b = order[p]
        return [
            slice(at, at + SUB)
            for t in range(SUB)
            for parity in range(2)
            for at in ((a * SUB + t) * cj + parity * ri + b * SUB,)
        ]

    for load in loads:
        load.wait()
    prepare_weights(0)
    prepare_columns(0)
    for a in range(groups):
        for b in range(groups):
            p = place[a, b]
            values = jnp.concatenate([x_in[rows, :] for rows in pieces(p)], axis=0).T
            state[:, lanes_of(p)] = values
            normalize_into(values, 0, a * groups + b, 0)
        side(0, 0, a * groups, groups, send_first, 2 * count, 2 * groups * a)
        side(0, 2, a * groups, groups, send_first, 2 * count, 2 * groups * a + groups)
        if a == 0:
            with jax.named_scope("barrier"):
                pl.semaphore_wait(barrier, slots - 1)
        with jax.named_scope("send_first"):
            send(send_first, have_first, 2 * count, 2 * groups * a, 2 * groups, a)
    for a in range(groups):
        gate = jax.nn.sigmoid(product(0, 4, 1, a * groups, groups))
        for b in range(groups):
            gating[:, lanes_of(place[a, b])] = gate[:, lanes_of(b)]
    prepare_weights(1)
    prepare_columns(1)
    mask = mask_in[...].astype(F32)
    for t in range(tokens // LANES):
        mask_rows[lanes_of(t), :] = columns_of(mask[t : t + 1, :])
    for a in range(groups):
        near = jnp.concatenate(
            [mask_rows[q * ri + a * SUB : q * ri + (a + 1) * SUB, :] for q in range(nr)], axis=0
        )
        mask_near[lanes_of(a), :] = near
        mask_lanes[a] = near.T[0:SUB, :]
        for t in range(SUB):
            for b8 in range(half):
                mask_far[pl.ds(a * span + t * nr + b8 * SUB, SUB), :] = mask_rows[
                    pl.ds(b8 * SUB * ri + a * SUB + t, SUB, stride=ri), :
                ]

    def send_blocks(first, number, buffer, have, sem, strided):
        for p in range(first, first + number):
            for b8 in range(half):
                if strided:
                    parts = [blocks[pl.ds(p * span + b8 * SUB * SUB + t, SUB, stride=SUB), :] for t in range(SUB)]
                else:
                    parts = [blocks[pl.ds(p * span + t * nr + b8 * SUB, SUB), :] for t in range(SUB)]
                to_owners(parts, buffer, count, p, b8)
        send(buffer, have, count, first, number, sem)

    def keep_blocks(values, firsts, seconds):
        for i, a in enumerate(firsts):
            for j, b in enumerate(seconds):
                blocks[lanes_of(place[a, b]), :] = values[i * span : (i + 1) * span, lanes_of(j)]

    near_groups = list(range(last))
    all_groups = list(range(groups))

    def far_times_near(firsts, seconds):
        values = lax.dot_general(
            left_cat[firsts[0] * span : (firsts[-1] + 1) * span, :],
            right_cat[seconds[0] * span : (seconds[-1] + 1) * span, :],
            (((1,), (1,)), ((), ())),
            preferred_element_type=F32,
        )
        keep_blocks(values, firsts, seconds)

    for a in range(groups):
        with jax.named_scope("wait_first"):
            await_bytes(have_first, 2 * groups, recv_sem, a)
        for b in range(groups):
            for b8 in range(half):
                for t, part in enumerate(at_owner(have_first, 2 * count, 2 * groups * a + b, b8)):
                    rows_a[pl.ds(b * span + t * nr + b8 * SUB, SUB), :] = part
                for t, part in enumerate(at_owner(have_first, 2 * count, 2 * groups * a + groups + b, b8)):
                    rows_b[pl.ds(b * span + b8 * SUB * SUB + t, SUB, stride=SUB), :] = part
        for b in range(groups):
            high, low = high_low(
                rows_a[lanes_of(b), :] * mask_lanes[b, 0:1, :] * mask_far[a * span : (a + 1) * span, :]
            )
            rows = slice(a * span, (a + 1) * span)
            left_cat[rows, lanes_of(b)] = high
            left_cat[rows, lanes_of(groups + b)] = low
            left_cat[rows, lanes_of(2 * groups + b)] = high
            high, low = high_low(rows_b[lanes_of(b), :] * mask_near[lanes_of(a), :])
            right_cat[rows, lanes_of(b)] = high
            right_cat[rows, lanes_of(groups + b)] = high
            right_cat[rows, lanes_of(2 * groups + b)] = low
        if a == last - 1:
            far_times_near(near_groups, near_groups)
            with jax.named_scope("send_mixed"):
                send_blocks(0, cut_a, send_mixed, have_mixed, groups, False)
    far_times_near([last], near_groups)
    far_times_near(all_groups, [last])
    with jax.named_scope("send_mixed"):
        send_blocks(cut_a, count - cut_a, send_mixed, have_mixed, groups + 1, False)

    def project_second(first, number, sem):
        side(1, 0, 0, number, send_second, 2 * count, 2 * first)
        side(1, 2, 0, number, send_second, 2 * count, 2 * first + number)
        with jax.named_scope("send_second"):
            send(send_second, have_second, 2 * count, 2 * first, 2 * number, sem)
        gating[:, lanes_of(first, number)] = jax.nn.sigmoid(product(1, 4, 1, 0, number))

    second_sets = ((0, cut_a), (cut_a, cut_b), (cut_b, count))
    for i, (first, stop) in enumerate(second_sets):
        number = stop - first
        if i < 2:
            with jax.named_scope("wait_mixed"):
                await_bytes(have_mixed, (cut_a, count - cut_a)[i], recv_sem, groups + i)
        values = finish(0, first, number, have_mixed)
        state[:, lanes_of(first, number)] = values
        for t in range(number):
            normalize_into(state[:, lanes_of(first + t)], 1, t, 0)
        project_second(first, number, groups + 2 + i)

    def under_times(firsts, seconds):
        values = jnp.dot(
            left_cat[firsts[0] * span : (firsts[-1] + 1) * span, :],
            under_cat[:, seconds[0] * span : (seconds[-1] + 1) * span],
            preferred_element_type=F32,
        )
        keep_blocks(values, firsts, seconds)

    for i, (first, stop) in enumerate(second_sets):
        number = stop - first
        with jax.named_scope("wait_second"):
            await_bytes(have_second, 2 * number, recv_sem, groups + 2 + i)
        for p in range(first, stop):
            a, b = order[p]
            row = first + p
            for b8 in range(half):
                for t, part in enumerate(at_owner(have_second, 2 * count, row, b8)):
                    rows_a[pl.ds(t * nr + b8 * SUB, SUB), :] = part
                for t, part in enumerate(at_owner(have_second, 2 * count, row + number, b8)):
                    rows_b[pl.ds(t * nr + b8 * SUB, SUB), :] = part
            high, low = high_low((rows_a[0:span, :] * mask_lanes[b, 0:1, :]).T)
            rows = slice(b * span, (b + 1) * span)
            left_cat[rows, lanes_of(a)] = high
            left_cat[rows, lanes_of(groups + a)] = low
            left_cat[rows, lanes_of(2 * groups + a)] = high
            high, low = high_low(
                rows_b[0:span, :] * mask_lanes[b, 0:1, :] * mask_far[a * span : (a + 1) * span, :]
            )
            under_cat[lanes_of(a), lanes_of(b)] = high
            under_cat[lanes_of(groups + a), lanes_of(b)] = high
            under_cat[lanes_of(2 * groups + a), lanes_of(b)] = low
        if i == 1:
            under_times(near_groups, near_groups)
            with jax.named_scope("send_next"):
                send_blocks(0, cut_a, send_next, have_next, groups + 5, True)
    under_times([last], near_groups)
    under_times(all_groups, [last])
    with jax.named_scope("send_next"):
        send_blocks(cut_a, count - cut_a, send_next, have_next, groups + 6, True)
    for i, (first, stop) in enumerate(((0, cut_a), (cut_a, count))):
        with jax.named_scope("wait_next"):
            await_bytes(have_next, stop - first, recv_sem, groups + 5 + i)
        values = finish(1, first, stop - first, have_next)
        for p in range(first, stop):
            tile = values[:, lanes_of(p - first)].T
            for q, rows in enumerate(pieces(p)):
                y_ref[rows, :] = tile[q * SUB : (q + 1) * SUB, :]

    for a in range(groups):
        await_bytes(send_first, 2 * groups, send_sem, a)
    for i, rows in enumerate((cut_a, count - cut_a)):
        await_bytes(send_mixed, rows, send_sem, groups + i)
        await_bytes(send_next, rows, send_sem, groups + 5 + i)
    for i, (first, stop) in enumerate(second_sets):
        await_bytes(send_second, 2 * (stop - first), send_sem, groups + 2 + i)


def body(
    nr,
    nc,
    pair_state,
    token_mask,
    norm_gain,
    norm_bias,
    proj_weight,
    gate_weight,
    out_gain,
    out_bias,
    out_weight,
):
    ri, cj, channels = pair_state.shape
    hidden = proj_weight.shape[2] // 4
    tokens = token_mask.shape[0]
    slots = nr * nc
    positions = ri * cj
    assert slots == hidden == channels == LANES
    assert nc == SUB and nr == 2 * nc and cj == 2 * ri and tokens == nr * ri == nc * cj
    assert ri % SUB == 0 and ri > SUB and tokens % LANES == 0
    groups = ri // SUB
    count = groups * groups
    message = pltpu.VMEM((slots * count, LANES), F32)
    double = pltpu.VMEM((slots * 2 * count, LANES), F32)
    inputs = (
        pair_state.reshape(positions, channels),
        token_mask.reshape(tokens // LANES, LANES),
        norm_gain,
        norm_bias,
        proj_weight,
        gate_weight,
        out_gain,
        out_bias,
        out_weight,
    )
    result = pl.pallas_call(
        functools.partial(kernel, (nr, nc, ri, cj)),
        out_shape=jax.ShapeDtypeStruct((positions, channels), F32),
        in_specs=[pl.BlockSpec(memory_space=pltpu.HBM)] * len(inputs),
        out_specs=pl.BlockSpec(memory_space=pltpu.VMEM),
        scratch_shapes=[
            *(pltpu.VMEM(i.shape, i.dtype) for i in inputs),
            pltpu.VMEM((2, 6 * LANES, 3 * LANES), BF16),
            pltpu.VMEM((8, LANES, LANES), F32),
            pltpu.VMEM((tokens, LANES), F32),
            pltpu.VMEM((groups, SUB, LANES), F32),
            pltpu.VMEM((tokens, LANES), F32),
            pltpu.VMEM((tokens, LANES), F32),
            pltpu.VMEM((channels, positions), F32),
            pltpu.VMEM((channels, positions), F32),
            pltpu.VMEM((3 * LANES, positions), BF16),
            double,
            double,
            message,
            message,
            double,
            double,
            message,
            message,
            pltpu.VMEM((tokens, LANES), F32),
            pltpu.VMEM((tokens, LANES), F32),
            pltpu.VMEM((tokens, 3 * tokens), BF16),
            pltpu.VMEM((tokens, 3 * tokens), BF16),
            pltpu.VMEM((3 * tokens, tokens), BF16),
            pltpu.VMEM((count * LANES, LANES), F32),
            pltpu.SemaphoreType.DMA((len(inputs),)),
            pltpu.SemaphoreType.DMA((groups + 7,)),
            pltpu.SemaphoreType.DMA((groups + 7,)),
        ],
        compiler_params=pltpu.CompilerParams(
            collective_id=0, has_side_effects=True, vmem_limit_bytes=48 * 2**20
        ),
        name="triangles",
    )(*(pltpu.with_memory_space_constraint(i, pltpu.HBM) for i in inputs))
    return result.reshape(pair_state.shape)


def solution(mesh):
    placed = (P(("groups", "rows"), "cols", None), P("groups"), P(), P(), P(), P(), P(), P(), P())
    return jax.shard_map(
        functools.partial(body, mesh.shape["rows"], mesh.shape["cols"]),
        mesh=mesh,
        in_specs=placed,
        out_specs=P(("groups", "rows"), "cols", None),
        check_vma=False,
    )
```

```python
import functools

import jax
import jax.numpy as jnp
from jax import lax
from jax.experimental import pallas as pl
from jax.experimental.pallas import tpu as pltpu
from jax.sharding import PartitionSpec as P

MESH = pl.DeviceIdType.MESH
eps = 1e-05
LANES = 128
SUB = 8
F32 = jnp.float32
BF16 = jnp.bfloat16


def high_low(values):
    high = values.astype(BF16)
    low = (values - high.astype(F32)).astype(BF16)
    return high, low


def columns_of(row):
    return jnp.broadcast_to(row, (LANES, LANES)).T


def swap_blocks(parts):
    width = LANES // SUB
    block = lax.broadcasted_iota(jnp.int32, (SUB, LANES), 1) // width
    parts = list(parts)
    for step in (1, 2, 4):
        odd = (block // step) % 2 == 1
        for a in range(SUB):
            if (a // step) % 2 == 0:
                low, high = parts[a], parts[a + step]
                parts[a] = jnp.where(odd, pltpu.roll(high, step * width, 1), low)
                parts[a + step] = jnp.where(odd, high, pltpu.roll(low, LANES - step * width, 1))
    return parts


def kernel(
    sizes,
    x_hbm,
    mask_hbm,
    norm_gain_hbm,
    norm_bias_hbm,
    proj_hbm,
    gate_hbm,
    out_gain_hbm,
    out_bias_hbm,
    out_hbm,
    y_ref,
    x_in,
    mask_in,
    norm_gain_in,
    norm_bias_in,
    proj_in,
    gate_in,
    out_gain_in,
    out_bias_in,
    out_in,
    weights,
    columns,
    mask_rows,
    mask_lanes,
    mask_near,
    mask_far,
    state,
    gating,
    normed,
    send_first,
    have_first,
    send_mixed,
    have_mixed,
    send_second,
    have_second,
    send_next,
    have_next,
    rows_a,
    rows_b,
    left_cat,
    right_cat,
    under_cat,
    blocks,
    load_sem,
    send_sem,
    recv_sem,
):
    nr, nc, ri, cj = sizes
    slots = nr * nc
    groups = ri // SUB
    half = nr // SUB
    tokens = nr * ri
    span = SUB * nr
    last = groups - 1
    early = [(a, b) for a in range(last) for b in range(last)]
    order = early + [(last, b) for b in range(last)] + [(a, last) for a in range(groups)]
    count = len(order)
    cut_a, cut_b = len(early), len(early) + last
    place = {ab: p for p, ab in enumerate(order)}

    r, c = lax.axis_index("rows"), lax.axis_index("cols")
    me = c * nr + r
    pair, core = r // 2, lax.rem(r, 2)
    pairs = nr // 2
    cols = [lax.rem(c + d, nc) for d in range(nc)]
    cores = [core, 1 - core]
    rows_at = [lax.rem(pair + d, pairs) * 2 for d in range(pairs)]
    turns = [d for d in (4, 1, 7, 2, 6, 3, 5, 0) if d < nc]

    loads = [
        pltpu.make_async_copy(src, dst, load_sem.at[i])
        for i, (src, dst) in enumerate(
            (
                (x_hbm, x_in),
                (norm_gain_hbm, norm_gain_in),
                (norm_bias_hbm, norm_bias_in),
                (proj_hbm, proj_in),
                (mask_hbm, mask_in),
                (gate_hbm, gate_in),
                (out_gain_hbm, out_gain_in),
                (out_bias_hbm, out_bias_in),
                (out_hbm, out_in),
            )
        )
    ]
    for load in loads:
        load.start()

    def to_all(act, how):
        def mixed(i, carry):
            turned = []
            for d in range(pairs):
                far = lax.rem(i + d, pairs)
                turned.append((far, lax.rem(pair + far, pairs) * 2))
            for dx in turns:
                for k in range(2):
                    far, base = turned[(dx + 4 * k) % pairs]
                    row = base + cores[k]

                    def go(row=row, dx=dx):
                        act(cols[dx] * nr + row, {"rows": row, "cols": cols[dx]})

                    if dx == 0 and k == 0:
                        pl.when(far != 0)(go)
                    else:
                        go()
            return carry

        def far_first(i, carry):
            turn, odd = i // 2, lax.rem(i, 2)
            away = pairs // 2 + turn - odd * (2 * turn + 1)
            far_row = lax.rem(pair + away, pairs) * 2
            far_col = lax.rem(c + away, nc)
            for d in turns:
                for k in range(2):
                    row, col = (far_row + cores[0], cols[d]) if k == 0 else (rows_at[d] + cores[1], far_col)

                    def go(row=row, col=col):
                        act(col * nr + row, {"rows": row, "cols": col})

                    if d == 0 and k == 0:
                        pl.when(away != 0)(go)
                    else:
                        go()
            return carry

        def by_row(i, carry):
            for d in turns:
                for k in range(2):
                    row = i * 2 + cores[k]

                    def go(row=row, d=d):
                        act(cols[d] * nr + row, {"rows": row, "cols": cols[d]})

                    if d == 0 and k == 0:
                        pl.when(i != pair)(go)
                    else:
                        go()
            return carry

        lax.fori_loop(0, pairs, {"mixed": mixed, "far": far_first, "row": by_row}[how], 0)

    barrier = pltpu.get_barrier_semaphore()
    to_all(lambda slot, device: pl.semaphore_signal(barrier, inc=1, device_id=device, device_id_type=MESH), "far")

    def send(src, dst, stride, base, rows, sem, how="mixed"):
        def act(slot, device):
            pltpu.make_async_remote_copy(
                src_ref=src.at[pl.ds(slot * stride + base, rows)],
                dst_ref=dst.at[pl.ds(me * stride + base, rows)],
                send_sem=send_sem.at[sem],
                recv_sem=recv_sem.at[sem],
                device_id=device,
                device_id_type=MESH,
            ).start()

        to_all(act, how)
        for q in range(rows):
            dst[pl.ds(me * stride + base + q, 1), :] = src[pl.ds(me * stride + base + q, 1), :]

    def await_bytes(buffer, rows, sems, sem):
        whole = buffer.at[pl.ds(0, (slots - 1) * rows)]
        pltpu.make_async_copy(whole, whole, sems.at[sem]).wait()

    def prepare_weights(u):
        def one(values, at):
            high, low = high_low(values.T)
            rows = pl.ds(at * LANES, LANES)
            weights[u, rows, 0:LANES] = high
            weights[u, rows, LANES : 2 * LANES] = low
            weights[u, rows, 2 * LANES : 3 * LANES] = high

        for f in range(4):
            one(proj_in[u, :, f * LANES : (f + 1) * LANES], f)
        one(gate_in[u], 4)
        one(out_in[u], 5)

    def prepare_columns(u):
        for i, ref in enumerate((norm_gain_in, norm_bias_in, out_gain_in, out_bias_in)):
            columns[4 * u + i] = columns_of(ref[pl.ds(u, 1), :])

    def lanes_of(first, number=1):
        return slice(first * LANES, (first + number) * LANES)

    def normalize(values, gain, bias):
        center = values - jnp.mean(values, axis=0, keepdims=True)
        spread = jnp.mean(center * center, axis=0, keepdims=True)
        return center * lax.rsqrt(spread + eps) * gain + bias

    def normalize_into(values, u, at, first):
        high, low = high_low(normalize(values, columns[4 * u + first], columns[4 * u + first + 1]))
        normed[0:LANES, lanes_of(at)] = high
        normed[LANES : 2 * LANES, lanes_of(at)] = high
        normed[2 * LANES : 3 * LANES, lanes_of(at)] = low

    def product(u, first, number, at, tiles):
        return jnp.dot(
            weights[u, first * LANES : (first + number) * LANES, :],
            normed[:, lanes_of(at, tiles)],
            preferred_element_type=F32,
        )

    def side(u, first, at, tiles, buffer, stride, base):
        hidden = product(u, first, 2, at, tiles)
        values = jax.nn.sigmoid(hidden[0:LANES]) * hidden[LANES:]
        for b in range(slots // SUB):
            for t in range(tiles):
                buffer[pl.ds(b * SUB * stride + base + t, SUB, stride=stride), :] = values[
                    b * SUB : (b + 1) * SUB, lanes_of(t)
                ]

    def at_owner(buffer, stride, row, b8):
        return swap_blocks(
            [buffer[pl.ds((a * nr + b8 * SUB) * stride + row, SUB, stride=stride), :] for a in range(nc)]
        )

    def to_owners(parts, buffer, stride, row, b8):
        for a, part in enumerate(swap_blocks(parts)):
            buffer[pl.ds((a * nr + b8 * SUB) * stride + row, SUB, stride=stride), :] = part

    def finish(u, first, number, have):
        for t in range(number):
            normalize_into(
                jnp.concatenate(
                    [have[pl.ds(b * SUB * count + first + t, SUB, stride=count), :] for b in range(slots // SUB)],
                    axis=0,
                ),
                u,
                t,
                2,
            )
        lanes = lanes_of(first, number)
        return state[:, lanes] + gating[:, lanes] * product(u, 5, 1, 0, number)

    def pieces(p):
        a, b = order[p]
        return [
            slice(at, at + SUB)
            for t in range(SUB)
            for parity in range(2)
            for at in ((a * SUB + t) * cj + parity * ri + b * SUB,)
        ]

    for load in loads:
        load.wait()
    prepare_weights(0)
    prepare_columns(0)
    for a in range(groups):
        for b in range(groups):
            p = place[a, b]
            values = jnp.concatenate([x_in[rows, :] for rows in pieces(p)], axis=0).T
            state[:, lanes_of(p)] = values
            normalize_into(values, 0, a * groups + b, 0)
        side(0, 0, a * groups, groups, send_first, 2 * count, 2 * groups * a)
        side(0, 2, a * groups, groups, send_first, 2 * count, 2 * groups * a + groups)
        if a == 0:
            with jax.named_scope("barrier"):
                pl.semaphore_wait(barrier, slots - 1)
        at = 2 * groups * a
        with jax.named_scope("send_first"):
            if a < last:
                send(send_first, have_first, 2 * count, at, 2 * groups, a)
            else:
                send(send_first, have_first, 2 * count, at, groups, a)
                send(send_first, have_first, 2 * count, at + groups, groups, a + 1)
    for a in range(groups):
        gate = jax.nn.sigmoid(product(0, 4, 1, a * groups, groups))
        for b in range(groups):
            gating[:, lanes_of(place[a, b])] = gate[:, lanes_of(b)]
    prepare_weights(1)
    prepare_columns(1)
    mask = mask_in[...].astype(F32)
    for t in range(tokens // LANES):
        mask_rows[lanes_of(t), :] = columns_of(mask[t : t + 1, :])
    for a in range(groups):
        near = jnp.concatenate(
            [mask_rows[q * ri + a * SUB : q * ri + (a + 1) * SUB, :] for q in range(nr)], axis=0
        )
        mask_near[lanes_of(a), :] = near
        mask_lanes[a] = near.T[0:SUB, :]
        for t in range(SUB):
            for b8 in range(half):
                mask_far[pl.ds(a * span + t * nr + b8 * SUB, SUB), :] = mask_rows[
                    pl.ds(b8 * SUB * ri + a * SUB + t, SUB, stride=ri), :
                ]

    def send_blocks(first, number, buffer, have, sem, strided, how="mixed"):
        for p in range(first, first + number):
            for b8 in range(half):
                if strided:
                    parts = [blocks[pl.ds(p * span + b8 * SUB * SUB + t, SUB, stride=SUB), :] for t in range(SUB)]
                else:
                    parts = [blocks[pl.ds(p * span + t * nr + b8 * SUB, SUB), :] for t in range(SUB)]
                to_owners(parts, buffer, count, p, b8)
        send(buffer, have, count, first, number, sem, how)

    def keep_blocks(values, firsts, seconds):
        for i, a in enumerate(firsts):
            for j, b in enumerate(seconds):
                blocks[lanes_of(place[a, b]), :] = values[i * span : (i + 1) * span, lanes_of(j)]

    near_groups = list(range(last))
    all_groups = list(range(groups))

    def far_times_near(firsts, seconds):
        values = lax.dot_general(
            left_cat[firsts[0] * span : (firsts[-1] + 1) * span, :],
            right_cat[seconds[0] * span : (seconds[-1] + 1) * span, :],
            (((1,), (1,)), ((), ())),
            preferred_element_type=F32,
        )
        keep_blocks(values, firsts, seconds)

    def take_left(a):
        rows = slice(a * span, (a + 1) * span)
        for b in range(groups):
            for b8 in range(half):
                for t, part in enumerate(at_owner(have_first, 2 * count, 2 * groups * a + b, b8)):
                    rows_a[pl.ds(b * span + t * nr + b8 * SUB, SUB), :] = part
        for b in range(groups):
            high, low = high_low(rows_a[lanes_of(b), :] * mask_lanes[b, 0:1, :] * mask_far[rows, :])
            left_cat[rows, lanes_of(b)] = high
            left_cat[rows, lanes_of(groups + b)] = low
            left_cat[rows, lanes_of(2 * groups + b)] = high

    def take_right(a):
        rows = slice(a * span, (a + 1) * span)
        for b in range(groups):
            for b8 in range(half):
                for t, part in enumerate(at_owner(have_first, 2 * count, 2 * groups * a + groups + b, b8)):
                    rows_b[pl.ds(b * span + b8 * SUB * SUB + t, SUB, stride=SUB), :] = part
        for b in range(groups):
            high, low = high_low(rows_b[lanes_of(b), :] * mask_near[lanes_of(a), :])
            right_cat[rows, lanes_of(b)] = high
            right_cat[rows, lanes_of(groups + b)] = high
            right_cat[rows, lanes_of(2 * groups + b)] = low

    def await_first(rows, sem):
        with jax.named_scope("wait_first"):
            await_bytes(have_first, rows, recv_sem, sem)

    def send_mixed_tiles(first, stop, sem):
        with jax.named_scope("send_mixed"):
            send_blocks(first, stop - first, send_mixed, have_mixed, sem, False)

    for a in range(last):
        await_first(2 * groups, a)
        take_left(a)
        take_right(a)
    far_times_near(near_groups, near_groups)
    send_mixed_tiles(0, cut_a, groups + 1)
    await_first(groups, last)
    take_left(last)
    far_times_near([last], near_groups)
    send_mixed_tiles(cut_a, cut_b, groups + 2)
    await_first(groups, groups)
    take_right(last)
    far_times_near(all_groups, [last])
    send_mixed_tiles(cut_b, count, groups + 3)

    sets = ((0, cut_a), (cut_a, cut_b), (cut_b, count))
    for i, (first, stop) in enumerate(sets):
        number = stop - first
        with jax.named_scope("wait_mixed"):
            await_bytes(have_mixed, number, recv_sem, groups + 1 + i)
        values = finish(0, first, number, have_mixed)
        state[:, lanes_of(first, number)] = values
        for t in range(number):
            normalize_into(state[:, lanes_of(first + t)], 1, t, 0)
        side(1, 0, 0, number, send_second, 2 * count, 2 * first)
        if i == 2:
            with jax.named_scope("send_second"):
                send(send_second, have_second, 2 * count, 2 * first, number, groups + 4 + i)
        side(1, 2, 0, number, send_second, 2 * count, 2 * first + number)
        with jax.named_scope("send_second"):
            if i == 2:
                send(send_second, have_second, 2 * count, 2 * first + number, number, groups + 5 + i)
            else:
                send(send_second, have_second, 2 * count, 2 * first, 2 * number, groups + 4 + i)
        gating[:, lanes_of(first, number)] = jax.nn.sigmoid(product(1, 4, 1, 0, number))

    def under_times(firsts, seconds):
        values = jnp.dot(
            left_cat[firsts[0] * span : (firsts[-1] + 1) * span, :],
            under_cat[:, seconds[0] * span : (seconds[-1] + 1) * span],
            preferred_element_type=F32,
        )
        keep_blocks(values, firsts, seconds)

    def take_under_left(first, stop):
        for p in range(first, stop):
            a, b = order[p]
            for b8 in range(half):
                for t, part in enumerate(at_owner(have_second, 2 * count, first + p, b8)):
                    rows_a[pl.ds(t * nr + b8 * SUB, SUB), :] = part
            high, low = high_low((rows_a[0:span, :] * mask_lanes[b, 0:1, :]).T)
            rows = slice(b * span, (b + 1) * span)
            left_cat[rows, lanes_of(a)] = high
            left_cat[rows, lanes_of(groups + a)] = low
            left_cat[rows, lanes_of(2 * groups + a)] = high

    def take_under_right(first, stop):
        for p in range(first, stop):
            a, b = order[p]
            for b8 in range(half):
                for t, part in enumerate(at_owner(have_second, 2 * count, p + stop, b8)):
                    rows_b[pl.ds(t * nr + b8 * SUB, SUB), :] = part
            high, low = high_low(
                rows_b[0:span, :] * mask_lanes[b, 0:1, :] * mask_far[a * span : (a + 1) * span, :]
            )
            under_cat[lanes_of(a), lanes_of(b)] = high
            under_cat[lanes_of(groups + a), lanes_of(b)] = high
            under_cat[lanes_of(2 * groups + a), lanes_of(b)] = low

    def await_second(rows, sem):
        with jax.named_scope("wait_second"):
            await_bytes(have_second, rows, recv_sem, sem)

    def send_next_tiles(first, stop, sem, how):
        with jax.named_scope("send_next"):
            send_blocks(first, stop - first, send_next, have_next, sem, True, how)

    for i in range(2):
        first, stop = sets[i]
        await_second(2 * (stop - first), groups + 4 + i)
        take_under_left(first, stop)
        take_under_right(first, stop)
    under_times(near_groups, near_groups)
    send_next_tiles(0, cut_a, groups + 8, "mixed")
    await_second(groups, groups + 6)
    take_under_left(cut_b, count)
    under_times([last], near_groups)
    send_next_tiles(cut_a, cut_b, groups + 9, "row")
    await_second(groups, groups + 7)
    take_under_right(cut_b, count)
    under_times(all_groups, [last])
    send_next_tiles(cut_b, count, groups + 10, "row")
    for i, (first, stop) in enumerate(sets):
        with jax.named_scope("wait_next"):
            await_bytes(have_next, stop - first, recv_sem, groups + 8 + i)
        values = finish(1, first, stop - first, have_next)
        for p in range(first, stop):
            tile = values[:, lanes_of(p - first)].T
            for q, rows in enumerate(pieces(p)):
                y_ref[rows, :] = tile[q * SUB : (q + 1) * SUB, :]

    for a in range(last):
        await_bytes(send_first, 2 * groups, send_sem, a)
    for part in range(2):
        await_bytes(send_first, groups, send_sem, last + part)
        await_bytes(send_second, groups, send_sem, groups + 6 + part)
    for i, (first, stop) in enumerate(sets):
        await_bytes(send_mixed, stop - first, send_sem, groups + 1 + i)
        await_bytes(send_next, stop - first, send_sem, groups + 8 + i)
        if i < 2:
            await_bytes(send_second, 2 * (stop - first), send_sem, groups + 4 + i)


def body(
    nr,
    nc,
    pair_state,
    token_mask,
    norm_gain,
    norm_bias,
    proj_weight,
    gate_weight,
    out_gain,
    out_bias,
    out_weight,
):
    ri, cj, channels = pair_state.shape
    hidden = proj_weight.shape[2] // 4
    tokens = token_mask.shape[0]
    slots = nr * nc
    positions = ri * cj
    assert slots == hidden == channels == LANES
    assert nc == SUB and nr == 2 * nc and cj == 2 * ri and tokens == nr * ri == nc * cj
    assert ri % SUB == 0 and ri > SUB and tokens % LANES == 0
    groups = ri // SUB
    count = groups * groups
    message = pltpu.VMEM((slots * count, LANES), F32)
    double = pltpu.VMEM((slots * 2 * count, LANES), F32)
    inputs = (
        pair_state.reshape(positions, channels),
        token_mask.reshape(tokens // LANES, LANES),
        norm_gain,
        norm_bias,
        proj_weight,
        gate_weight,
        out_gain,
        out_bias,
        out_weight,
    )
    result = pl.pallas_call(
        functools.partial(kernel, (nr, nc, ri, cj)),
        out_shape=jax.ShapeDtypeStruct((positions, channels), F32),
        in_specs=[pl.BlockSpec(memory_space=pltpu.HBM)] * len(inputs),
        out_specs=pl.BlockSpec(memory_space=pltpu.VMEM),
        scratch_shapes=[
            *(pltpu.VMEM(i.shape, i.dtype) for i in inputs),
            pltpu.VMEM((2, 6 * LANES, 3 * LANES), BF16),
            pltpu.VMEM((8, LANES, LANES), F32),
            pltpu.VMEM((tokens, LANES), F32),
            pltpu.VMEM((groups, SUB, LANES), F32),
            pltpu.VMEM((tokens, LANES), F32),
            pltpu.VMEM((tokens, LANES), F32),
            pltpu.VMEM((channels, positions), F32),
            pltpu.VMEM((channels, positions), F32),
            pltpu.VMEM((3 * LANES, positions), BF16),
            double,
            double,
            message,
            message,
            double,
            double,
            message,
            message,
            pltpu.VMEM((tokens, LANES), F32),
            pltpu.VMEM((tokens, LANES), F32),
            pltpu.VMEM((tokens, 3 * tokens), BF16),
            pltpu.VMEM((tokens, 3 * tokens), BF16),
            pltpu.VMEM((3 * tokens, tokens), BF16),
            pltpu.VMEM((count * LANES, LANES), F32),
            pltpu.SemaphoreType.DMA((len(inputs),)),
            pltpu.SemaphoreType.DMA((groups + 11,)),
            pltpu.SemaphoreType.DMA((groups + 11,)),
        ],
        compiler_params=pltpu.CompilerParams(
            collective_id=0, has_side_effects=True, vmem_limit_bytes=48 * 2**20
        ),
        name="triangles",
    )(*(pltpu.with_memory_space_constraint(i, pltpu.HBM) for i in inputs))
    return result.reshape(pair_state.shape)


def solution(mesh):
    placed = (P(("groups", "rows"), "cols", None), P("groups"), P(), P(), P(), P(), P(), P(), P())
    return jax.shard_map(
        functools.partial(body, mesh.shape["rows"], mesh.shape["cols"]),
        mesh=mesh,
        in_specs=placed,
        out_specs=P(("groups", "rows"), "cols", None),
        check_vma=False,
    )
```

```python
import functools

import jax
import jax.numpy as jnp
from jax import lax
from jax.experimental import pallas as pl
from jax.experimental.pallas import tpu as pltpu
from jax.sharding import PartitionSpec as P

MESH = pl.DeviceIdType.MESH
eps = 1e-05
LANES = 128
SUB = 8
F32 = jnp.float32
BF16 = jnp.bfloat16


def high_low(values):
    high = values.astype(BF16)
    low = (values - high.astype(F32)).astype(BF16)
    return high, low


def columns_of(row):
    return jnp.broadcast_to(row, (LANES, LANES)).T


def swap_blocks(parts):
    width = LANES // SUB
    block = lax.broadcasted_iota(jnp.int32, (SUB, LANES), 1) // width
    parts = list(parts)
    for step in (1, 2, 4):
        odd = (block // step) % 2 == 1
        for a in range(SUB):
            if (a // step) % 2 == 0:
                low, high = parts[a], parts[a + step]
                parts[a] = jnp.where(odd, pltpu.roll(high, step * width, 1), low)
                parts[a + step] = jnp.where(odd, high, pltpu.roll(low, LANES - step * width, 1))
    return parts


def kernel(
    sizes,
    x_hbm,
    mask_hbm,
    norm_gain_hbm,
    norm_bias_hbm,
    proj_hbm,
    gate_hbm,
    out_gain_hbm,
    out_bias_hbm,
    out_hbm,
    y_ref,
    x_in,
    mask_in,
    norm_gain_in,
    norm_bias_in,
    proj_in,
    gate_in,
    out_gain_in,
    out_bias_in,
    out_in,
    weights,
    columns,
    mask_rows,
    mask_lanes,
    mask_near,
    mask_far,
    state,
    gating,
    normed,
    send_first,
    have_first,
    send_mixed,
    have_mixed,
    send_second,
    have_second,
    send_next,
    have_next,
    rows_a,
    rows_b,
    left_cat,
    right_cat,
    under_cat,
    blocks,
    load_sem,
    send_sem,
    recv_sem,
    ready,
):
    nr, nc, ri, cj = sizes
    slots = nr * nc
    groups = ri // SUB
    half = nr // SUB
    tokens = nr * ri
    span = SUB * nr
    last = groups - 1
    early = [(a, b) for a in range(last) for b in range(last)]
    order = early + [(last, b) for b in range(last)] + [(a, last) for a in range(groups)]
    count = len(order)
    cut_a, cut_b = len(early), len(early) + last
    place = {ab: p for p, ab in enumerate(order)}

    r, c = lax.axis_index("rows"), lax.axis_index("cols")
    me = c * nr + r
    pair, core = r // 2, lax.rem(r, 2)
    pairs = nr // 2
    cols = [lax.rem(c + d, nc) for d in range(nc)]
    cores = [core, 1 - core]
    rows_at = [lax.rem(pair + d, pairs) * 2 for d in range(pairs)]
    turns = [d for d in (4, 1, 7, 2, 6, 3, 5, 0) if d < nc]

    loads = [
        pltpu.make_async_copy(src, dst, load_sem.at[i])
        for i, (src, dst) in enumerate(
            (
                (x_hbm, x_in),
                (norm_gain_hbm, norm_gain_in),
                (norm_bias_hbm, norm_bias_in),
                (proj_hbm, proj_in),
                (mask_hbm, mask_in),
                (gate_hbm, gate_in),
                (out_gain_hbm, out_gain_in),
                (out_bias_hbm, out_bias_in),
                (out_hbm, out_in),
            )
        )
    ]
    for load in loads:
        load.start()

    def to_all(act, how):
        def mixed(i, carry):
            turned = []
            for d in range(pairs):
                far = lax.rem(i + d, pairs)
                turned.append((far, lax.rem(pair + far, pairs) * 2))
            for dx in turns:
                for k in range(2):
                    far, base = turned[(dx + 4 * k) % pairs]
                    row = base + cores[k]

                    def go(row=row, dx=dx):
                        act(cols[dx] * nr + row, {"rows": row, "cols": cols[dx]})

                    if dx == 0 and k == 0:
                        pl.when(far != 0)(go)
                    else:
                        go()
            return carry

        def far_first(i, carry):
            turn, odd = i // 2, lax.rem(i, 2)
            away = pairs // 2 + turn - odd * (2 * turn + 1)
            far_row = lax.rem(pair + away, pairs) * 2
            far_col = lax.rem(c + away, nc)
            for d in turns:
                for k in range(2):
                    row, col = (far_row + cores[0], cols[d]) if k == 0 else (rows_at[d] + cores[1], far_col)

                    def go(row=row, col=col):
                        act(col * nr + row, {"rows": row, "cols": col})

                    if d == 0 and k == 0:
                        pl.when(away != 0)(go)
                    else:
                        go()
            return carry

        def by_row(i, carry):
            for d in turns:
                for k in range(2):
                    row = i * 2 + cores[k]

                    def go(row=row, d=d):
                        act(cols[d] * nr + row, {"rows": row, "cols": cols[d]})

                    if d == 0 and k == 0:
                        pl.when(i != pair)(go)
                    else:
                        go()
            return carry

        lax.fori_loop(0, pairs, {"mixed": mixed, "far": far_first, "row": by_row}[how], 0)

    barrier = pltpu.get_barrier_semaphore()

    def greet(semaphore):
        to_all(
            lambda slot, device: pl.semaphore_signal(semaphore, inc=1, device_id=device, device_id_type=MESH), "far"
        )

    @pl.when(me != 0)
    def _():
        greet(barrier)

    @pl.when(me == 0)
    def _():
        pl.semaphore_wait(barrier, slots - 1)
        greet(ready)

    def copy_to(src, dst, stride, base, rows, sem):
        def act(slot, device):
            pltpu.make_async_remote_copy(
                src_ref=src.at[pl.ds(slot * stride + base, rows)],
                dst_ref=dst.at[pl.ds(me * stride + base, rows)],
                send_sem=send_sem.at[sem],
                recv_sem=recv_sem.at[sem],
                device_id=device,
                device_id_type=MESH,
            ).start()

        return act

    def keep_own(src, dst, stride, base, rows):
        for q in range(rows):
            dst[pl.ds(me * stride + base + q, 1), :] = src[pl.ds(me * stride + base + q, 1), :]

    def send(src, dst, stride, base, rows, sem, how="mixed"):
        to_all(copy_to(src, dst, stride, base, rows, sem), how)
        keep_own(src, dst, stride, base, rows)

    def await_bytes(buffer, rows, sems, sem):
        whole = buffer.at[pl.ds(0, (slots - 1) * rows)]
        pltpu.make_async_copy(whole, whole, sems.at[sem]).wait()

    def prepare_weights(u):
        def one(values, at):
            high, low = high_low(values.T)
            rows = pl.ds(at * LANES, LANES)
            weights[u, rows, 0:LANES] = high
            weights[u, rows, LANES : 2 * LANES] = low
            weights[u, rows, 2 * LANES : 3 * LANES] = high

        for f in range(4):
            one(proj_in[u, :, f * LANES : (f + 1) * LANES], f)
        one(gate_in[u], 4)
        one(out_in[u], 5)

    def prepare_columns(u):
        for i, ref in enumerate((norm_gain_in, norm_bias_in, out_gain_in, out_bias_in)):
            columns[4 * u + i] = columns_of(ref[pl.ds(u, 1), :])

    def lanes_of(first, number=1):
        return slice(first * LANES, (first + number) * LANES)

    def normalize(values, gain, bias):
        center = values - jnp.mean(values, axis=0, keepdims=True)
        spread = jnp.mean(center * center, axis=0, keepdims=True)
        return center * lax.rsqrt(spread + eps) * gain + bias

    def normalize_into(values, u, at, first):
        high, low = high_low(normalize(values, columns[4 * u + first], columns[4 * u + first + 1]))
        normed[0:LANES, lanes_of(at)] = high
        normed[LANES : 2 * LANES, lanes_of(at)] = high
        normed[2 * LANES : 3 * LANES, lanes_of(at)] = low

    def product(u, first, number, at, tiles):
        return jnp.dot(
            weights[u, first * LANES : (first + number) * LANES, :],
            normed[:, lanes_of(at, tiles)],
            preferred_element_type=F32,
        )

    def side(u, first, at, tiles, buffer, stride, base):
        hidden = product(u, first, 2, at, tiles)
        values = jax.nn.sigmoid(hidden[0:LANES]) * hidden[LANES:]
        for b in range(slots // SUB):
            for t in range(tiles):
                buffer[pl.ds(b * SUB * stride + base + t, SUB, stride=stride), :] = values[
                    b * SUB : (b + 1) * SUB, lanes_of(t)
                ]

    def at_owner(buffer, stride, row, b8):
        return swap_blocks(
            [buffer[pl.ds((a * nr + b8 * SUB) * stride + row, SUB, stride=stride), :] for a in range(nc)]
        )

    def to_owners(parts, buffer, stride, row, b8):
        for a, part in enumerate(swap_blocks(parts)):
            buffer[pl.ds((a * nr + b8 * SUB) * stride + row, SUB, stride=stride), :] = part

    def finish(u, first, number, have):
        for t in range(number):
            normalize_into(
                jnp.concatenate(
                    [have[pl.ds(b * SUB * count + first + t, SUB, stride=count), :] for b in range(slots // SUB)],
                    axis=0,
                ),
                u,
                t,
                2,
            )
        lanes = lanes_of(first, number)
        return state[:, lanes] + gating[:, lanes] * product(u, 5, 1, 0, number)

    def pieces(p):
        a, b = order[p]
        return [
            slice(at, at + SUB)
            for t in range(SUB)
            for parity in range(2)
            for at in ((a * SUB + t) * cj + parity * ri + b * SUB,)
        ]

    for load in loads:
        load.wait()
    prepare_weights(0)
    prepare_columns(0)
    for a in range(groups):
        for b in range(groups):
            p = place[a, b]
            values = jnp.concatenate([x_in[rows, :] for rows in pieces(p)], axis=0).T
            state[:, lanes_of(p)] = values
            normalize_into(values, 0, a * groups + b, 0)
        side(0, 0, a * groups, groups, send_first, 2 * count, 2 * groups * a)
        side(0, 2, a * groups, groups, send_first, 2 * count, 2 * groups * a + groups)
        at = 2 * groups * a
        if a == 0:
            with jax.named_scope("send_first"):
                copy = copy_to(send_first, have_first, 2 * count, at, 2 * groups, a)

                @pl.when(me == 0)
                def _():
                    to_all(copy, "mixed")

                @pl.when(me != 0)
                def _():
                    pl.semaphore_wait(barrier, slots - 2)
                    to_all(lambda slot, device: pl.when(slot != 0)(lambda: copy(slot, device)), "mixed")
                    pl.semaphore_wait(ready, 1)
                    copy(0, {"rows": 0, "cols": 0})

                keep_own(send_first, have_first, 2 * count, at, 2 * groups)
            continue
        with jax.named_scope("send_first"):
            if a < last:
                send(send_first, have_first, 2 * count, at, 2 * groups, a)
            else:
                send(send_first, have_first, 2 * count, at, groups, a)
                send(send_first, have_first, 2 * count, at + groups, groups, a + 1)
    for a in range(groups):
        gate = jax.nn.sigmoid(product(0, 4, 1, a * groups, groups))
        for b in range(groups):
            gating[:, lanes_of(place[a, b])] = gate[:, lanes_of(b)]
    prepare_weights(1)
    prepare_columns(1)
    mask = mask_in[...].astype(F32)
    for t in range(tokens // LANES):
        mask_rows[lanes_of(t), :] = columns_of(mask[t : t + 1, :])
    for a in range(groups):
        near = jnp.concatenate(
            [mask_rows[q * ri + a * SUB : q * ri + (a + 1) * SUB, :] for q in range(nr)], axis=0
        )
        mask_near[lanes_of(a), :] = near
        mask_lanes[a] = near.T[0:SUB, :]
        for t in range(SUB):
            for b8 in range(half):
                mask_far[pl.ds(a * span + t * nr + b8 * SUB, SUB), :] = mask_rows[
                    pl.ds(b8 * SUB * ri + a * SUB + t, SUB, stride=ri), :
                ]

    def send_blocks(first, number, buffer, have, sem, strided, how="mixed"):
        for p in range(first, first + number):
            for b8 in range(half):
                if strided:
                    parts = [blocks[pl.ds(p * span + b8 * SUB * SUB + t, SUB, stride=SUB), :] for t in range(SUB)]
                else:
                    parts = [blocks[pl.ds(p * span + t * nr + b8 * SUB, SUB), :] for t in range(SUB)]
                to_owners(parts, buffer, count, p, b8)
        send(buffer, have, count, first, number, sem, how)

    def keep_blocks(values, firsts, seconds):
        for i, a in enumerate(firsts):
            for j, b in enumerate(seconds):
                blocks[lanes_of(place[a, b]), :] = values[i * span : (i + 1) * span, lanes_of(j)]

    near_groups = list(range(last))
    all_groups = list(range(groups))

    def far_times_near(firsts, seconds):
        values = lax.dot_general(
            left_cat[firsts[0] * span : (firsts[-1] + 1) * span, :],
            right_cat[seconds[0] * span : (seconds[-1] + 1) * span, :],
            (((1,), (1,)), ((), ())),
            preferred_element_type=F32,
        )
        keep_blocks(values, firsts, seconds)

    def take_left(a):
        rows = slice(a * span, (a + 1) * span)
        for b in range(groups):
            for b8 in range(half):
                for t, part in enumerate(at_owner(have_first, 2 * count, 2 * groups * a + b, b8)):
                    rows_a[pl.ds(b * span + t * nr + b8 * SUB, SUB), :] = part
        for b in range(groups):
            high, low = high_low(rows_a[lanes_of(b), :] * mask_lanes[b, 0:1, :] * mask_far[rows, :])
            left_cat[rows, lanes_of(b)] = high
            left_cat[rows, lanes_of(groups + b)] = low
            left_cat[rows, lanes_of(2 * groups + b)] = high

    def take_right(a):
        rows = slice(a * span, (a + 1) * span)
        for b in range(groups):
            for b8 in range(half):
                for t, part in enumerate(at_owner(have_first, 2 * count, 2 * groups * a + groups + b, b8)):
                    rows_b[pl.ds(b * span + b8 * SUB * SUB + t, SUB, stride=SUB), :] = part
        for b in range(groups):
            high, low = high_low(rows_b[lanes_of(b), :] * mask_near[lanes_of(a), :])
            right_cat[rows, lanes_of(b)] = high
            right_cat[rows, lanes_of(groups + b)] = high
            right_cat[rows, lanes_of(2 * groups + b)] = low

    def await_first(rows, sem):
        with jax.named_scope("wait_first"):
            await_bytes(have_first, rows, recv_sem, sem)

    def send_mixed_tiles(first, stop, sem):
        with jax.named_scope("send_mixed"):
            send_blocks(first, stop - first, send_mixed, have_mixed, sem, False)

    for a in range(last):
        await_first(2 * groups, a)
        take_left(a)
        take_right(a)
    far_times_near(near_groups, near_groups)
    send_mixed_tiles(0, cut_a, groups + 1)
    await_first(groups, last)
    take_left(last)
    far_times_near([last], near_groups)
    send_mixed_tiles(cut_a, cut_b, groups + 2)
    await_first(groups, groups)
    take_right(last)
    far_times_near(all_groups, [last])
    send_mixed_tiles(cut_b, count, groups + 3)

    sets = ((0, cut_a), (cut_a, cut_b), (cut_b, count))
    for i, (first, stop) in enumerate(sets):
        number = stop - first
        with jax.named_scope("wait_mixed"):
            await_bytes(have_mixed, number, recv_sem, groups + 1 + i)
        values = finish(0, first, number, have_mixed)
        state[:, lanes_of(first, number)] = values
        for t in range(number):
            normalize_into(state[:, lanes_of(first + t)], 1, t, 0)
        side(1, 0, 0, number, send_second, 2 * count, 2 * first)
        if i == 2:
            with jax.named_scope("send_second"):
                send(send_second, have_second, 2 * count, 2 * first, number, groups + 4 + i)
        side(1, 2, 0, number, send_second, 2 * count, 2 * first + number)
        with jax.named_scope("send_second"):
            if i == 2:
                send(send_second, have_second, 2 * count, 2 * first + number, number, groups + 5 + i)
            else:
                send(send_second, have_second, 2 * count, 2 * first, 2 * number, groups + 4 + i)
        gating[:, lanes_of(first, number)] = jax.nn.sigmoid(product(1, 4, 1, 0, number))

    def under_times(firsts, seconds):
        values = jnp.dot(
            left_cat[firsts[0] * span : (firsts[-1] + 1) * span, :],
            under_cat[:, seconds[0] * span : (seconds[-1] + 1) * span],
            preferred_element_type=F32,
        )
        keep_blocks(values, firsts, seconds)

    def take_under_left(first, stop):
        for p in range(first, stop):
            a, b = order[p]
            for b8 in range(half):
                for t, part in enumerate(at_owner(have_second, 2 * count, first + p, b8)):
                    rows_a[pl.ds(t * nr + b8 * SUB, SUB), :] = part
            high, low = high_low((rows_a[0:span, :] * mask_lanes[b, 0:1, :]).T)
            rows = slice(b * span, (b + 1) * span)
            left_cat[rows, lanes_of(a)] = high
            left_cat[rows, lanes_of(groups + a)] = low
            left_cat[rows, lanes_of(2 * groups + a)] = high

    def take_under_right(first, stop):
        for p in range(first, stop):
            a, b = order[p]
            for b8 in range(half):
                for t, part in enumerate(at_owner(have_second, 2 * count, p + stop, b8)):
                    rows_b[pl.ds(t * nr + b8 * SUB, SUB), :] = part
            high, low = high_low(
                rows_b[0:span, :] * mask_lanes[b, 0:1, :] * mask_far[a * span : (a + 1) * span, :]
            )
            under_cat[lanes_of(a), lanes_of(b)] = high
            under_cat[lanes_of(groups + a), lanes_of(b)] = high
            under_cat[lanes_of(2 * groups + a), lanes_of(b)] = low

    def await_second(rows, sem):
        with jax.named_scope("wait_second"):
            await_bytes(have_second, rows, recv_sem, sem)

    def send_next_tiles(first, stop, sem, how):
        with jax.named_scope("send_next"):
            send_blocks(first, stop - first, send_next, have_next, sem, True, how)

    for i in range(2):
        first, stop = sets[i]
        await_second(2 * (stop - first), groups + 4 + i)
        take_under_left(first, stop)
        take_under_right(first, stop)
    under_times(near_groups, near_groups)
    send_next_tiles(0, cut_a, groups + 8, "mixed")
    await_second(groups, groups + 6)
    take_under_left(cut_b, count)
    under_times([last], near_groups)
    send_next_tiles(cut_a, cut_b, groups + 9, "row")
    await_second(groups, groups + 7)
    take_under_right(cut_b, count)
    under_times(all_groups, [last])
    send_next_tiles(cut_b, count, groups + 10, "row")
    for i, (first, stop) in enumerate(sets):
        with jax.named_scope("wait_next"):
            await_bytes(have_next, stop - first, recv_sem, groups + 8 + i)
        values = finish(1, first, stop - first, have_next)
        for p in range(first, stop):
            tile = values[:, lanes_of(p - first)].T
            for q, rows in enumerate(pieces(p)):
                y_ref[rows, :] = tile[q * SUB : (q + 1) * SUB, :]

    for a in range(last):
        await_bytes(send_first, 2 * groups, send_sem, a)
    for part in range(2):
        await_bytes(send_first, groups, send_sem, last + part)
        await_bytes(send_second, groups, send_sem, groups + 6 + part)
    for i, (first, stop) in enumerate(sets):
        await_bytes(send_mixed, stop - first, send_sem, groups + 1 + i)
        await_bytes(send_next, stop - first, send_sem, groups + 8 + i)
        if i < 2:
            await_bytes(send_second, 2 * (stop - first), send_sem, groups + 4 + i)


def body(
    nr,
    nc,
    pair_state,
    token_mask,
    norm_gain,
    norm_bias,
    proj_weight,
    gate_weight,
    out_gain,
    out_bias,
    out_weight,
):
    ri, cj, channels = pair_state.shape
    hidden = proj_weight.shape[2] // 4
    tokens = token_mask.shape[0]
    slots = nr * nc
    positions = ri * cj
    assert slots == hidden == channels == LANES
    assert nc == SUB and nr == 2 * nc and cj == 2 * ri and tokens == nr * ri == nc * cj
    assert ri % SUB == 0 and ri > SUB and tokens % LANES == 0
    groups = ri // SUB
    count = groups * groups
    message = pltpu.VMEM((slots * count, LANES), F32)
    double = pltpu.VMEM((slots * 2 * count, LANES), F32)
    inputs = (
        pair_state.reshape(positions, channels),
        token_mask.reshape(tokens // LANES, LANES),
        norm_gain,
        norm_bias,
        proj_weight,
        gate_weight,
        out_gain,
        out_bias,
        out_weight,
    )
    result = pl.pallas_call(
        functools.partial(kernel, (nr, nc, ri, cj)),
        out_shape=jax.ShapeDtypeStruct((positions, channels), F32),
        in_specs=[pl.BlockSpec(memory_space=pltpu.HBM)] * len(inputs),
        out_specs=pl.BlockSpec(memory_space=pltpu.VMEM),
        scratch_shapes=[
            *(pltpu.VMEM(i.shape, i.dtype) for i in inputs),
            pltpu.VMEM((2, 6 * LANES, 3 * LANES), BF16),
            pltpu.VMEM((8, LANES, LANES), F32),
            pltpu.VMEM((tokens, LANES), F32),
            pltpu.VMEM((groups, SUB, LANES), F32),
            pltpu.VMEM((tokens, LANES), F32),
            pltpu.VMEM((tokens, LANES), F32),
            pltpu.VMEM((channels, positions), F32),
            pltpu.VMEM((channels, positions), F32),
            pltpu.VMEM((3 * LANES, positions), BF16),
            double,
            double,
            message,
            message,
            double,
            double,
            message,
            message,
            pltpu.VMEM((tokens, LANES), F32),
            pltpu.VMEM((tokens, LANES), F32),
            pltpu.VMEM((tokens, 3 * tokens), BF16),
            pltpu.VMEM((tokens, 3 * tokens), BF16),
            pltpu.VMEM((3 * tokens, tokens), BF16),
            pltpu.VMEM((count * LANES, LANES), F32),
            pltpu.SemaphoreType.DMA((len(inputs),)),
            pltpu.SemaphoreType.DMA((groups + 11,)),
            pltpu.SemaphoreType.DMA((groups + 11,)),
            pltpu.SemaphoreType.REGULAR,
        ],
        compiler_params=pltpu.CompilerParams(
            collective_id=0, has_side_effects=True, vmem_limit_bytes=48 * 2**20
        ),
        name="triangles",
    )(*(pltpu.with_memory_space_constraint(i, pltpu.HBM) for i in inputs))
    return result.reshape(pair_state.shape)


def solution(mesh):
    placed = (P(("groups", "rows"), "cols", None), P("groups"), P(), P(), P(), P(), P(), P(), P())
    return jax.shard_map(
        functools.partial(body, mesh.shape["rows"], mesh.shape["cols"]),
        mesh=mesh,
        in_specs=placed,
        out_specs=P(("groups", "rows"), "cols", None),
        check_vma=False,
    )
```

```python
import functools

import jax
import jax.numpy as jnp
from jax import lax
from jax.experimental import pallas as pl
from jax.experimental.pallas import tpu as pltpu
from jax.sharding import PartitionSpec as P

MESH = pl.DeviceIdType.MESH
eps = 1e-05
LANES = 128
SUB = 8
F32 = jnp.float32
BF16 = jnp.bfloat16


def high_low(values):
    high = values.astype(BF16)
    low = (values - high.astype(F32)).astype(BF16)
    return high, low


def columns_of(row):
    return jnp.broadcast_to(row, (LANES, LANES)).T


def swap_blocks(parts):
    width = LANES // SUB
    block = lax.broadcasted_iota(jnp.int32, (SUB, LANES), 1) // width
    parts = list(parts)
    for step in (1, 2, 4):
        odd = (block // step) % 2 == 1
        for a in range(SUB):
            if (a // step) % 2 == 0:
                low, high = parts[a], parts[a + step]
                parts[a] = jnp.where(odd, pltpu.roll(high, step * width, 1), low)
                parts[a + step] = jnp.where(odd, high, pltpu.roll(low, LANES - step * width, 1))
    return parts


def kernel(
    sizes,
    x_hbm,
    mask_hbm,
    norm_gain_hbm,
    norm_bias_hbm,
    proj_hbm,
    gate_hbm,
    out_gain_hbm,
    out_bias_hbm,
    out_hbm,
    y_ref,
    x_in,
    mask_in,
    norm_gain_in,
    norm_bias_in,
    proj_in,
    gate_in,
    out_gain_in,
    out_bias_in,
    out_in,
    weights,
    columns,
    mask_rows,
    mask_lanes,
    mask_near,
    mask_far,
    state,
    gating,
    normed,
    send_first,
    have_first,
    send_mixed,
    have_mixed,
    send_second,
    have_second,
    send_next,
    have_next,
    rows_a,
    rows_b,
    left_cat,
    right_cat,
    under_cat,
    blocks,
    load_sem,
    send_sem,
    recv_sem,
    ready,
):
    nr, nc, ri, cj = sizes
    slots = nr * nc
    groups = ri // SUB
    half = nr // SUB
    tokens = nr * ri
    span = SUB * nr
    last = groups - 1
    early = [(a, b) for a in range(last) for b in range(last)]
    order = early + [(last, b) for b in range(last)] + [(a, last) for a in range(groups)]
    count = len(order)
    cut_a, cut_b = len(early), len(early) + last
    place = {ab: p for p, ab in enumerate(order)}

    r, c = lax.axis_index("rows"), lax.axis_index("cols")
    me = c * nr + r
    pair, core = r // 2, lax.rem(r, 2)
    pairs = nr // 2
    cols = [lax.rem(c + d, nc) for d in range(nc)]
    cores = [core, 1 - core]
    rows_at = [lax.rem(pair + d, pairs) * 2 for d in range(pairs)]
    turns = [d for d in (4, 1, 7, 2, 6, 3, 5, 0) if d < nc]

    loads = [
        pltpu.make_async_copy(src, dst, load_sem.at[i])
        for i, (src, dst) in enumerate(
            (
                (x_hbm, x_in),
                (norm_gain_hbm, norm_gain_in),
                (norm_bias_hbm, norm_bias_in),
                (proj_hbm, proj_in),
                (mask_hbm, mask_in),
                (gate_hbm, gate_in),
                (out_gain_hbm, out_gain_in),
                (out_bias_hbm, out_bias_in),
                (out_hbm, out_in),
            )
        )
    ]
    for load in loads:
        load.start()

    def to_all(act, how):
        def mixed(i, carry):
            turned = []
            for d in range(pairs):
                far = lax.rem(i + d, pairs)
                turned.append((far, lax.rem(pair + far, pairs) * 2))
            for dx in turns:
                for k in range(2):
                    far, base = turned[(dx + 4 * k) % pairs]
                    row = base + cores[k]

                    def go(row=row, dx=dx):
                        act(cols[dx] * nr + row, {"rows": row, "cols": cols[dx]})

                    if dx == 0 and k == 0:
                        pl.when(far != 0)(go)
                    else:
                        go()
            return carry

        def far_first(i, carry):
            turn, odd = i // 2, lax.rem(i, 2)
            away = pairs // 2 + turn - odd * (2 * turn + 1)
            far_row = lax.rem(pair + away, pairs) * 2
            far_col = lax.rem(c + away, nc)
            for d in turns:
                for k in range(2):
                    row, col = (far_row + cores[0], cols[d]) if k == 0 else (rows_at[d] + cores[1], far_col)

                    def go(row=row, col=col):
                        act(col * nr + row, {"rows": row, "cols": col})

                    if d == 0 and k == 0:
                        pl.when(away != 0)(go)
                    else:
                        go()
            return carry

        def by_row(i, carry):
            for d in sorted(turns, key=lambda d: -min(d, nc - d)):
                for k in range(2):
                    row = i * 2 + cores[k]

                    def go(row=row, d=d):
                        act(cols[d] * nr + row, {"rows": row, "cols": cols[d]})

                    if d == 0 and k == 0:
                        pl.when(i != pair)(go)
                    else:
                        go()
            return carry

        lax.fori_loop(0, pairs, {"mixed": mixed, "far": far_first, "row": by_row}[how], 0)

    barrier = pltpu.get_barrier_semaphore()

    def greet(semaphore):
        to_all(
            lambda slot, device: pl.semaphore_signal(semaphore, inc=1, device_id=device, device_id_type=MESH), "far"
        )

    @pl.when(me != 0)
    def _():
        greet(barrier)

    @pl.when(me == 0)
    def _():
        pl.semaphore_wait(barrier, slots - 1)
        greet(ready)

    def copy_to(src, dst, stride, base, rows, sem):
        def act(slot, device):
            pltpu.make_async_remote_copy(
                src_ref=src.at[pl.ds(slot * stride + base, rows)],
                dst_ref=dst.at[pl.ds(me * stride + base, rows)],
                send_sem=send_sem.at[sem],
                recv_sem=recv_sem.at[sem],
                device_id=device,
                device_id_type=MESH,
            ).start()

        return act

    def keep_own(src, dst, stride, base, rows):
        for q in range(rows):
            dst[pl.ds(me * stride + base + q, 1), :] = src[pl.ds(me * stride + base + q, 1), :]

    def send(src, dst, stride, base, rows, sem, how="mixed"):
        to_all(copy_to(src, dst, stride, base, rows, sem), how)
        keep_own(src, dst, stride, base, rows)

    def await_bytes(buffer, rows, sems, sem):
        whole = buffer.at[pl.ds(0, (slots - 1) * rows)]
        pltpu.make_async_copy(whole, whole, sems.at[sem]).wait()

    def prepare_weights(u):
        def one(values, at):
            high, low = high_low(values.T)
            rows = pl.ds(at * LANES, LANES)
            weights[u, rows, 0:LANES] = high
            weights[u, rows, LANES : 2 * LANES] = low
            weights[u, rows, 2 * LANES : 3 * LANES] = high

        for f in range(4):
            one(proj_in[u, :, f * LANES : (f + 1) * LANES], f)
        one(gate_in[u], 4)
        one(out_in[u], 5)

    def prepare_columns(u):
        for i, ref in enumerate((norm_gain_in, norm_bias_in, out_gain_in, out_bias_in)):
            columns[4 * u + i] = columns_of(ref[pl.ds(u, 1), :])

    def lanes_of(first, number=1):
        return slice(first * LANES, (first + number) * LANES)

    def normalize(values, gain, bias):
        center = values - jnp.mean(values, axis=0, keepdims=True)
        spread = jnp.mean(center * center, axis=0, keepdims=True)
        return center * lax.rsqrt(spread + eps) * gain + bias

    def normalize_into(values, u, at, first):
        high, low = high_low(normalize(values, columns[4 * u + first], columns[4 * u + first + 1]))
        normed[0:LANES, lanes_of(at)] = high
        normed[LANES : 2 * LANES, lanes_of(at)] = high
        normed[2 * LANES : 3 * LANES, lanes_of(at)] = low

    def product(u, first, number, at, tiles):
        return jnp.dot(
            weights[u, first * LANES : (first + number) * LANES, :],
            normed[:, lanes_of(at, tiles)],
            preferred_element_type=F32,
        )

    def side(u, first, at, tiles, buffer, stride, base):
        hidden = product(u, first, 2, at, tiles)
        values = jax.nn.sigmoid(hidden[0:LANES]) * hidden[LANES:]
        for b in range(slots // SUB):
            for t in range(tiles):
                buffer[pl.ds(b * SUB * stride + base + t, SUB, stride=stride), :] = values[
                    b * SUB : (b + 1) * SUB, lanes_of(t)
                ]

    def at_owner(buffer, stride, row, b8):
        return swap_blocks(
            [buffer[pl.ds((a * nr + b8 * SUB) * stride + row, SUB, stride=stride), :] for a in range(nc)]
        )

    def to_owners(parts, buffer, stride, row, b8):
        for a, part in enumerate(swap_blocks(parts)):
            buffer[pl.ds((a * nr + b8 * SUB) * stride + row, SUB, stride=stride), :] = part

    def finish(u, first, number, have):
        for t in range(number):
            normalize_into(
                jnp.concatenate(
                    [have[pl.ds(b * SUB * count + first + t, SUB, stride=count), :] for b in range(slots // SUB)],
                    axis=0,
                ),
                u,
                t,
                2,
            )
        lanes = lanes_of(first, number)
        return state[:, lanes] + gating[:, lanes] * product(u, 5, 1, 0, number)

    def pieces(p):
        a, b = order[p]
        return [
            slice(at, at + SUB)
            for t in range(SUB)
            for parity in range(2)
            for at in ((a * SUB + t) * cj + parity * ri + b * SUB,)
        ]

    for load in loads:
        load.wait()
    prepare_weights(0)
    prepare_columns(0)
    for a in range(groups):
        for b in range(groups):
            p = place[a, b]
            values = jnp.concatenate([x_in[rows, :] for rows in pieces(p)], axis=0).T
            state[:, lanes_of(p)] = values
            normalize_into(values, 0, a * groups + b, 0)
        side(0, 0, a * groups, groups, send_first, 2 * count, 2 * groups * a)
        side(0, 2, a * groups, groups, send_first, 2 * count, 2 * groups * a + groups)
        at = 2 * groups * a
        if a == 0:
            with jax.named_scope("send_first"):
                copy = copy_to(send_first, have_first, 2 * count, at, 2 * groups, a)

                @pl.when(me == 0)
                def _():
                    to_all(copy, "mixed")

                @pl.when(me != 0)
                def _():
                    pl.semaphore_wait(barrier, slots - 2)
                    to_all(lambda slot, device: pl.when(slot != 0)(lambda: copy(slot, device)), "mixed")
                    pl.semaphore_wait(ready, 1)
                    copy(0, {"rows": 0, "cols": 0})

                keep_own(send_first, have_first, 2 * count, at, 2 * groups)
            continue
        with jax.named_scope("send_first"):
            if a < last:
                send(send_first, have_first, 2 * count, at, 2 * groups, a)
            else:
                send(send_first, have_first, 2 * count, at, groups, a)
                send(send_first, have_first, 2 * count, at + groups, groups, a + 1)
    for a in range(groups):
        gate = jax.nn.sigmoid(product(0, 4, 1, a * groups, groups))
        for b in range(groups):
            gating[:, lanes_of(place[a, b])] = gate[:, lanes_of(b)]
    prepare_weights(1)
    prepare_columns(1)
    mask = mask_in[...].astype(F32)
    for t in range(tokens // LANES):
        mask_rows[lanes_of(t), :] = columns_of(mask[t : t + 1, :])
    for a in range(groups):
        near = jnp.concatenate(
            [mask_rows[q * ri + a * SUB : q * ri + (a + 1) * SUB, :] for q in range(nr)], axis=0
        )
        mask_near[lanes_of(a), :] = near
        mask_lanes[a] = near.T[0:SUB, :]
        for t in range(SUB):
            for b8 in range(half):
                mask_far[pl.ds(a * span + t * nr + b8 * SUB, SUB), :] = mask_rows[
                    pl.ds(b8 * SUB * ri + a * SUB + t, SUB, stride=ri), :
                ]

    def send_blocks(first, number, buffer, have, sem, strided, how="mixed"):
        for p in range(first, first + number):
            for b8 in range(half):
                if strided:
                    parts = [blocks[pl.ds(p * span + b8 * SUB * SUB + t, SUB, stride=SUB), :] for t in range(SUB)]
                else:
                    parts = [blocks[pl.ds(p * span + t * nr + b8 * SUB, SUB), :] for t in range(SUB)]
                to_owners(parts, buffer, count, p, b8)
        send(buffer, have, count, first, number, sem, how)

    def keep_blocks(values, firsts, seconds):
        for i, a in enumerate(firsts):
            for j, b in enumerate(seconds):
                blocks[lanes_of(place[a, b]), :] = values[i * span : (i + 1) * span, lanes_of(j)]

    near_groups = list(range(last))
    all_groups = list(range(groups))

    def far_times_near(firsts, seconds):
        values = lax.dot_general(
            left_cat[firsts[0] * span : (firsts[-1] + 1) * span, :],
            right_cat[seconds[0] * span : (seconds[-1] + 1) * span, :],
            (((1,), (1,)), ((), ())),
            preferred_element_type=F32,
        )
        keep_blocks(values, firsts, seconds)

    def take_left(a):
        rows = slice(a * span, (a + 1) * span)
        for b in range(groups):
            for b8 in range(half):
                for t, part in enumerate(at_owner(have_first, 2 * count, 2 * groups * a + b, b8)):
                    rows_a[pl.ds(b * span + t * nr + b8 * SUB, SUB), :] = part
        for b in range(groups):
            high, low = high_low(rows_a[lanes_of(b), :] * mask_lanes[b, 0:1, :] * mask_far[rows, :])
            left_cat[rows, lanes_of(b)] = high
            left_cat[rows, lanes_of(groups + b)] = low
            left_cat[rows, lanes_of(2 * groups + b)] = high

    def take_right(a):
        rows = slice(a * span, (a + 1) * span)
        for b in range(groups):
            for b8 in range(half):
                for t, part in enumerate(at_owner(have_first, 2 * count, 2 * groups * a + groups + b, b8)):
                    rows_b[pl.ds(b * span + b8 * SUB * SUB + t, SUB, stride=SUB), :] = part
        for b in range(groups):
            high, low = high_low(rows_b[lanes_of(b), :] * mask_near[lanes_of(a), :])
            right_cat[rows, lanes_of(b)] = high
            right_cat[rows, lanes_of(groups + b)] = high
            right_cat[rows, lanes_of(2 * groups + b)] = low

    def await_first(rows, sem):
        with jax.named_scope("wait_first"):
            await_bytes(have_first, rows, recv_sem, sem)

    def send_mixed_tiles(first, stop, sem):
        with jax.named_scope("send_mixed"):
            send_blocks(first, stop - first, send_mixed, have_mixed, sem, False)

    for a in range(last):
        await_first(2 * groups, a)
        take_left(a)
        take_right(a)
    far_times_near(near_groups, near_groups)
    send_mixed_tiles(0, cut_a, groups + 1)
    await_first(groups, last)
    take_left(last)
    far_times_near([last], near_groups)
    send_mixed_tiles(cut_a, cut_b, groups + 2)
    await_first(groups, groups)
    take_right(last)
    far_times_near(all_groups, [last])
    send_mixed_tiles(cut_b, count, groups + 3)

    sets = ((0, cut_a), (cut_a, cut_b), (cut_b, count))
    for i, (first, stop) in enumerate(sets):
        number = stop - first
        with jax.named_scope("wait_mixed"):
            await_bytes(have_mixed, number, recv_sem, groups + 1 + i)
        values = finish(0, first, number, have_mixed)
        state[:, lanes_of(first, number)] = values
        for t in range(number):
            normalize_into(state[:, lanes_of(first + t)], 1, t, 0)
        side(1, 0, 0, number, send_second, 2 * count, 2 * first)
        if i == 2:
            with jax.named_scope("send_second"):
                send(send_second, have_second, 2 * count, 2 * first, number, groups + 4 + i)
        side(1, 2, 0, number, send_second, 2 * count, 2 * first + number)
        with jax.named_scope("send_second"):
            if i == 2:
                send(send_second, have_second, 2 * count, 2 * first + number, number, groups + 5 + i, "far")
            else:
                send(send_second, have_second, 2 * count, 2 * first, 2 * number, groups + 4 + i)
        gating[:, lanes_of(first, number)] = jax.nn.sigmoid(product(1, 4, 1, 0, number))

    def under_times(firsts, seconds):
        values = jnp.dot(
            left_cat[firsts[0] * span : (firsts[-1] + 1) * span, :],
            under_cat[:, seconds[0] * span : (seconds[-1] + 1) * span],
            preferred_element_type=F32,
        )
        keep_blocks(values, firsts, seconds)

    def take_under_left(first, stop):
        for p in range(first, stop):
            a, b = order[p]
            for b8 in range(half):
                for t, part in enumerate(at_owner(have_second, 2 * count, first + p, b8)):
                    rows_a[pl.ds(t * nr + b8 * SUB, SUB), :] = part
            high, low = high_low((rows_a[0:span, :] * mask_lanes[b, 0:1, :]).T)
            rows = slice(b * span, (b + 1) * span)
            left_cat[rows, lanes_of(a)] = high
            left_cat[rows, lanes_of(groups + a)] = low
            left_cat[rows, lanes_of(2 * groups + a)] = high

    def take_under_right(first, stop):
        for p in range(first, stop):
            a, b = order[p]
            for b8 in range(half):
                for t, part in enumerate(at_owner(have_second, 2 * count, p + stop, b8)):
                    rows_b[pl.ds(t * nr + b8 * SUB, SUB), :] = part
            high, low = high_low(
                rows_b[0:span, :] * mask_lanes[b, 0:1, :] * mask_far[a * span : (a + 1) * span, :]
            )
            under_cat[lanes_of(a), lanes_of(b)] = high
            under_cat[lanes_of(groups + a), lanes_of(b)] = high
            under_cat[lanes_of(2 * groups + a), lanes_of(b)] = low

    def await_second(rows, sem):
        with jax.named_scope("wait_second"):
            await_bytes(have_second, rows, recv_sem, sem)

    def send_next_tiles(first, stop, sem, how):
        with jax.named_scope("send_next"):
            send_blocks(first, stop - first, send_next, have_next, sem, True, how)

    for i in range(2):
        first, stop = sets[i]
        await_second(2 * (stop - first), groups + 4 + i)
        take_under_left(first, stop)
        take_under_right(first, stop)
    under_times(near_groups, near_groups)
    send_next_tiles(0, cut_a, groups + 8, "far")
    await_second(groups, groups + 6)
    take_under_left(cut_b, count)
    under_times([last], near_groups)
    send_next_tiles(cut_a, cut_b, groups + 9, "row")
    await_second(groups, groups + 7)
    take_under_right(cut_b, count)
    under_times(all_groups, [last])
    send_next_tiles(cut_b, count, groups + 10, "row")
    for i, (first, stop) in enumerate(sets):
        with jax.named_scope("wait_next"):
            await_bytes(have_next, stop - first, recv_sem, groups + 8 + i)
        values = finish(1, first, stop - first, have_next)
        for p in range(first, stop):
            tile = values[:, lanes_of(p - first)].T
            for q, rows in enumerate(pieces(p)):
                y_ref[rows, :] = tile[q * SUB : (q + 1) * SUB, :]

    for a in range(last):
        await_bytes(send_first, 2 * groups, send_sem, a)
    for part in range(2):
        await_bytes(send_first, groups, send_sem, last + part)
        await_bytes(send_second, groups, send_sem, groups + 6 + part)
    for i, (first, stop) in enumerate(sets):
        await_bytes(send_mixed, stop - first, send_sem, groups + 1 + i)
        await_bytes(send_next, stop - first, send_sem, groups + 8 + i)
        if i < 2:
            await_bytes(send_second, 2 * (stop - first), send_sem, groups + 4 + i)


def body(
    nr,
    nc,
    pair_state,
    token_mask,
    norm_gain,
    norm_bias,
    proj_weight,
    gate_weight,
    out_gain,
    out_bias,
    out_weight,
):
    ri, cj, channels = pair_state.shape
    hidden = proj_weight.shape[2] // 4
    tokens = token_mask.shape[0]
    slots = nr * nc
    positions = ri * cj
    assert slots == hidden == channels == LANES
    assert nc == SUB and nr == 2 * nc and cj == 2 * ri and tokens == nr * ri == nc * cj
    assert ri % SUB == 0 and ri > SUB and tokens % LANES == 0
    groups = ri // SUB
    count = groups * groups
    message = pltpu.VMEM((slots * count, LANES), F32)
    double = pltpu.VMEM((slots * 2 * count, LANES), F32)
    inputs = (
        pair_state.reshape(positions, channels),
        token_mask.reshape(tokens // LANES, LANES),
        norm_gain,
        norm_bias,
        proj_weight,
        gate_weight,
        out_gain,
        out_bias,
        out_weight,
    )
    result = pl.pallas_call(
        functools.partial(kernel, (nr, nc, ri, cj)),
        out_shape=jax.ShapeDtypeStruct((positions, channels), F32),
        in_specs=[pl.BlockSpec(memory_space=pltpu.HBM)] * len(inputs),
        out_specs=pl.BlockSpec(memory_space=pltpu.VMEM),
        scratch_shapes=[
            *(pltpu.VMEM(i.shape, i.dtype) for i in inputs),
            pltpu.VMEM((2, 6 * LANES, 3 * LANES), BF16),
            pltpu.VMEM((8, LANES, LANES), F32),
            pltpu.VMEM((tokens, LANES), F32),
            pltpu.VMEM((groups, SUB, LANES), F32),
            pltpu.VMEM((tokens, LANES), F32),
            pltpu.VMEM((tokens, LANES), F32),
            pltpu.VMEM((channels, positions), F32),
            pltpu.VMEM((channels, positions), F32),
            pltpu.VMEM((3 * LANES, positions), BF16),
            double,
            double,
            message,
            message,
            double,
            double,
            message,
            message,
            pltpu.VMEM((tokens, LANES), F32),
            pltpu.VMEM((tokens, LANES), F32),
            pltpu.VMEM((tokens, 3 * tokens), BF16),
            pltpu.VMEM((tokens, 3 * tokens), BF16),
            pltpu.VMEM((3 * tokens, tokens), BF16),
            pltpu.VMEM((count * LANES, LANES), F32),
            pltpu.SemaphoreType.DMA((len(inputs),)),
            pltpu.SemaphoreType.DMA((groups + 11,)),
            pltpu.SemaphoreType.DMA((groups + 11,)),
            pltpu.SemaphoreType.REGULAR,
        ],
        compiler_params=pltpu.CompilerParams(
            collective_id=0, has_side_effects=True, vmem_limit_bytes=48 * 2**20
        ),
        name="triangles",
    )(*(pltpu.with_memory_space_constraint(i, pltpu.HBM) for i in inputs))
    return result.reshape(pair_state.shape)


def solution(mesh):
    placed = (P(("groups", "rows"), "cols", None), P("groups"), P(), P(), P(), P(), P(), P(), P())
    return jax.shard_map(
        functools.partial(body, mesh.shape["rows"], mesh.shape["cols"]),
        mesh=mesh,
        in_specs=placed,
        out_specs=P(("groups", "rows"), "cols", None),
        check_vma=False,
    )
```

```python
import functools

import jax
import jax.numpy as jnp
from jax import lax
from jax.experimental import pallas as pl
from jax.experimental.pallas import tpu as pltpu
from jax.sharding import PartitionSpec as P

MESH = pl.DeviceIdType.MESH
eps = 1e-05
LANES = 128
SUB = 8
F32 = jnp.float32
BF16 = jnp.bfloat16


def high_low(values):
    high = values.astype(BF16)
    low = (values - high.astype(F32)).astype(BF16)
    return high, low


def columns_of(row):
    return jnp.broadcast_to(row, (LANES, LANES)).T


def swap_blocks(parts):
    width = LANES // SUB
    block = lax.broadcasted_iota(jnp.int32, (SUB, LANES), 1) // width
    parts = list(parts)
    for step in (1, 2, 4):
        odd = (block // step) % 2 == 1
        for a in range(SUB):
            if (a // step) % 2 == 0:
                low, high = parts[a], parts[a + step]
                parts[a] = jnp.where(odd, pltpu.roll(high, step * width, 1), low)
                parts[a + step] = jnp.where(odd, high, pltpu.roll(low, LANES - step * width, 1))
    return parts


def kernel(
    sizes,
    x_hbm,
    mask_hbm,
    norm_gain_hbm,
    norm_bias_hbm,
    proj_hbm,
    gate_hbm,
    out_gain_hbm,
    out_bias_hbm,
    out_hbm,
    y_ref,
    x_in,
    mask_in,
    norm_gain_in,
    norm_bias_in,
    proj_in,
    gate_in,
    out_gain_in,
    out_bias_in,
    out_in,
    weights,
    columns,
    mask_rows,
    mask_lanes,
    mask_near,
    mask_far,
    state,
    gating,
    normed,
    send_first,
    have_first,
    send_mixed,
    have_mixed,
    send_second,
    have_second,
    send_next,
    have_next,
    rows_a,
    rows_b,
    left_cat,
    right_cat,
    under_cat,
    blocks,
    load_sem,
    send_sem,
    recv_sem,
    ready,
):
    nr, nc, ri, cj = sizes
    slots = nr * nc
    groups = ri // SUB
    half = nr // SUB
    tokens = nr * ri
    span = SUB * nr
    last = groups - 1
    early = [(a, b) for a in range(last) for b in range(last)]
    order = early + [(last, b) for b in range(last)] + [(a, last) for a in range(groups)]
    count = len(order)
    cut_a, cut_b = len(early), len(early) + last
    place = {ab: p for p, ab in enumerate(order)}

    r, c = lax.axis_index("rows"), lax.axis_index("cols")
    me = c * nr + r
    pair, core = r // 2, lax.rem(r, 2)
    pairs = nr // 2
    cols = [lax.rem(c + d, nc) for d in range(nc)]
    cores = [core, 1 - core]
    rows_at = [lax.rem(pair + d, pairs) * 2 for d in range(pairs)]
    turns = [d for d in (4, 1, 7, 2, 6, 3, 5, 0) if d < nc]

    loads = [
        pltpu.make_async_copy(src, dst, load_sem.at[i])
        for i, (src, dst) in enumerate(
            (
                (x_hbm, x_in),
                (norm_gain_hbm, norm_gain_in),
                (norm_bias_hbm, norm_bias_in),
                (proj_hbm, proj_in),
                (mask_hbm, mask_in),
                (gate_hbm, gate_in),
                (out_gain_hbm, out_gain_in),
                (out_bias_hbm, out_bias_in),
                (out_hbm, out_in),
            )
        )
    ]
    for load in loads:
        load.start()

    def to_all(act, how):
        def mixed(i, carry):
            turned = []
            for d in range(pairs):
                far = lax.rem(i + d, pairs)
                turned.append((far, lax.rem(pair + far, pairs) * 2))
            for dx in turns:
                for k in range(2):
                    far, base = turned[(dx + 4 * k) % pairs]
                    row = base + cores[k]

                    def go(row=row, dx=dx):
                        act(cols[dx] * nr + row, {"rows": row, "cols": cols[dx]})

                    if dx == 0 and k == 0:
                        pl.when(far != 0)(go)
                    else:
                        go()
            return carry

        def far_first(i, carry):
            turn, odd = i // 2, lax.rem(i, 2)
            away = pairs // 2 + turn - odd * (2 * turn + 1)
            far_row = lax.rem(pair + away, pairs) * 2
            far_col = lax.rem(c + away, nc)
            for d in turns:
                for k in range(2):
                    row, col = (far_row + cores[0], cols[d]) if k == 0 else (rows_at[d] + cores[1], far_col)

                    def go(row=row, col=col):
                        act(col * nr + row, {"rows": row, "cols": col})

                    if d == 0 and k == 0:
                        pl.when(away != 0)(go)
                    else:
                        go()
            return carry

        def by_row(i, carry):
            for d in sorted(turns, key=lambda d: -min(d, nc - d)):
                for k in range(2):
                    row = i * 2 + cores[k]

                    def go(row=row, d=d):
                        act(cols[d] * nr + row, {"rows": row, "cols": cols[d]})

                    if d == 0 and k == 0:
                        pl.when(i != pair)(go)
                    else:
                        go()
            return carry

        lax.fori_loop(0, pairs, {"mixed": mixed, "far": far_first, "row": by_row}[how], 0)

    barrier = pltpu.get_barrier_semaphore()

    def greet(semaphore):
        to_all(
            lambda slot, device: pl.semaphore_signal(semaphore, inc=1, device_id=device, device_id_type=MESH), "far"
        )

    @pl.when(me != 0)
    def _():
        greet(barrier)

    @pl.when(me == 0)
    def _():
        pl.semaphore_wait(barrier, slots - 1)
        greet(ready)

    def copy_to(src, dst, stride, base, rows, sem):
        def act(slot, device):
            pltpu.make_async_remote_copy(
                src_ref=src.at[pl.ds(slot * stride + base, rows)],
                dst_ref=dst.at[pl.ds(me * stride + base, rows)],
                send_sem=send_sem.at[sem],
                recv_sem=recv_sem.at[sem],
                device_id=device,
                device_id_type=MESH,
            ).start()

        return act

    def keep_own(src, dst, stride, base, rows):
        for q in range(rows):
            dst[pl.ds(me * stride + base + q, 1), :] = src[pl.ds(me * stride + base + q, 1), :]

    def send(src, dst, stride, base, rows, sem, how="mixed"):
        to_all(copy_to(src, dst, stride, base, rows, sem), how)
        keep_own(src, dst, stride, base, rows)

    def await_bytes(buffer, rows, sems, sem):
        whole = buffer.at[pl.ds(0, (slots - 1) * rows)]
        pltpu.make_async_copy(whole, whole, sems.at[sem]).wait()

    def prepare_weights(u):
        def one(values, at):
            high, low = high_low(values.T)
            rows = pl.ds(at * LANES, LANES)
            weights[u, rows, 0:LANES] = high
            weights[u, rows, LANES : 2 * LANES] = low
            weights[u, rows, 2 * LANES : 3 * LANES] = high

        for f in range(4):
            one(proj_in[u, :, f * LANES : (f + 1) * LANES], f)
        one(gate_in[u], 4)
        one(out_in[u], 5)

    def prepare_columns(u):
        for i, ref in enumerate((norm_gain_in, norm_bias_in, out_gain_in, out_bias_in)):
            columns[4 * u + i] = columns_of(ref[pl.ds(u, 1), :])

    def lanes_of(first, number=1):
        return slice(first * LANES, (first + number) * LANES)

    def normalize(values, gain, bias):
        center = values - jnp.mean(values, axis=0, keepdims=True)
        spread = jnp.mean(center * center, axis=0, keepdims=True)
        return center * lax.rsqrt(spread + eps) * gain + bias

    def normalize_into(values, u, at, first):
        high, low = high_low(normalize(values, columns[4 * u + first], columns[4 * u + first + 1]))
        normed[0:LANES, lanes_of(at)] = high
        normed[LANES : 2 * LANES, lanes_of(at)] = high
        normed[2 * LANES : 3 * LANES, lanes_of(at)] = low

    def product(u, first, number, at, tiles):
        return jnp.dot(
            weights[u, first * LANES : (first + number) * LANES, :],
            normed[:, lanes_of(at, tiles)],
            preferred_element_type=F32,
        )

    def side(u, first, at, tiles, buffer, stride, base):
        hidden = product(u, first, 2, at, tiles)
        values = jax.nn.sigmoid(hidden[0:LANES]) * hidden[LANES:]
        for b in range(slots // SUB):
            for t in range(tiles):
                buffer[pl.ds(b * SUB * stride + base + t, SUB, stride=stride), :] = values[
                    b * SUB : (b + 1) * SUB, lanes_of(t)
                ]

    def at_owner(buffer, stride, row, b8):
        return swap_blocks(
            [buffer[pl.ds((a * nr + b8 * SUB) * stride + row, SUB, stride=stride), :] for a in range(nc)]
        )

    def to_owners(parts, buffer, stride, row, b8):
        for a, part in enumerate(swap_blocks(parts)):
            buffer[pl.ds((a * nr + b8 * SUB) * stride + row, SUB, stride=stride), :] = part

    def finish(u, first, number, have):
        for t in range(number):
            normalize_into(
                jnp.concatenate(
                    [have[pl.ds(b * SUB * count + first + t, SUB, stride=count), :] for b in range(slots // SUB)],
                    axis=0,
                ),
                u,
                t,
                2,
            )
        lanes = lanes_of(first, number)
        return state[:, lanes] + gating[:, lanes] * product(u, 5, 1, 0, number)

    def pieces(p):
        a, b = order[p]
        return [
            slice(at, at + SUB)
            for t in range(SUB)
            for parity in range(2)
            for at in ((a * SUB + t) * cj + parity * ri + b * SUB,)
        ]

    for load in loads:
        load.wait()
    prepare_weights(0)
    prepare_columns(0)
    for a in range(groups):
        for b in range(groups):
            p = place[a, b]
            values = jnp.concatenate([x_in[rows, :] for rows in pieces(p)], axis=0).T
            state[:, lanes_of(p)] = values
            normalize_into(values, 0, a * groups + b, 0)
        side(0, 0, a * groups, groups, send_first, 2 * count, 2 * groups * a)
        side(0, 2, a * groups, groups, send_first, 2 * count, 2 * groups * a + groups)
        at = 2 * groups * a
        if a == 0:
            with jax.named_scope("send_first"):
                copy = copy_to(send_first, have_first, 2 * count, at, 2 * groups, a)

                @pl.when(me == 0)
                def _():
                    to_all(copy, "mixed")

                @pl.when(me != 0)
                def _():
                    pl.semaphore_wait(barrier, slots - 2)
                    to_all(lambda slot, device: pl.when(slot != 0)(lambda: copy(slot, device)), "mixed")
                    pl.semaphore_wait(ready, 1)
                    copy(0, {"rows": 0, "cols": 0})

                keep_own(send_first, have_first, 2 * count, at, 2 * groups)
            continue
        with jax.named_scope("send_first"):
            if a < last:
                send(send_first, have_first, 2 * count, at, 2 * groups, a)
            else:
                send(send_first, have_first, 2 * count, at, groups, a)
                send(send_first, have_first, 2 * count, at + groups, groups, a + 1, "far")
    for a in range(groups):
        gate = jax.nn.sigmoid(product(0, 4, 1, a * groups, groups))
        for b in range(groups):
            gating[:, lanes_of(place[a, b])] = gate[:, lanes_of(b)]
    prepare_weights(1)
    prepare_columns(1)
    mask = mask_in[...].astype(F32)
    for t in range(tokens // LANES):
        mask_rows[lanes_of(t), :] = columns_of(mask[t : t + 1, :])
    for a in range(groups):
        near = jnp.concatenate(
            [mask_rows[q * ri + a * SUB : q * ri + (a + 1) * SUB, :] for q in range(nr)], axis=0
        )
        mask_near[lanes_of(a), :] = near
        mask_lanes[a] = near.T[0:SUB, :]
        for t in range(SUB):
            for b8 in range(half):
                mask_far[pl.ds(a * span + t * nr + b8 * SUB, SUB), :] = mask_rows[
                    pl.ds(b8 * SUB * ri + a * SUB + t, SUB, stride=ri), :
                ]

    def send_blocks(first, number, buffer, have, sem, strided, how="mixed"):
        for p in range(first, first + number):
            for b8 in range(half):
                if strided:
                    parts = [blocks[pl.ds(p * span + b8 * SUB * SUB + t, SUB, stride=SUB), :] for t in range(SUB)]
                else:
                    parts = [blocks[pl.ds(p * span + t * nr + b8 * SUB, SUB), :] for t in range(SUB)]
                to_owners(parts, buffer, count, p, b8)
        send(buffer, have, count, first, number, sem, how)

    def keep_blocks(values, firsts, seconds):
        for i, a in enumerate(firsts):
            for j, b in enumerate(seconds):
                blocks[lanes_of(place[a, b]), :] = values[i * span : (i + 1) * span, lanes_of(j)]

    near_groups = list(range(last))
    all_groups = list(range(groups))

    def far_times_near(firsts, seconds):
        values = lax.dot_general(
            left_cat[firsts[0] * span : (firsts[-1] + 1) * span, :],
            right_cat[seconds[0] * span : (seconds[-1] + 1) * span, :],
            (((1,), (1,)), ((), ())),
            preferred_element_type=F32,
        )
        keep_blocks(values, firsts, seconds)

    def take_left(a):
        rows = slice(a * span, (a + 1) * span)
        for b in range(groups):
            for b8 in range(half):
                for t, part in enumerate(at_owner(have_first, 2 * count, 2 * groups * a + b, b8)):
                    rows_a[pl.ds(b * span + t * nr + b8 * SUB, SUB), :] = part
        for b in range(groups):
            high, low = high_low(rows_a[lanes_of(b), :] * mask_lanes[b, 0:1, :] * mask_far[rows, :])
            left_cat[rows, lanes_of(b)] = high
            left_cat[rows, lanes_of(groups + b)] = low
            left_cat[rows, lanes_of(2 * groups + b)] = high

    def take_right(a):
        rows = slice(a * span, (a + 1) * span)
        for b in range(groups):
            for b8 in range(half):
                for t, part in enumerate(at_owner(have_first, 2 * count, 2 * groups * a + groups + b, b8)):
                    rows_b[pl.ds(b * span + b8 * SUB * SUB + t, SUB, stride=SUB), :] = part
        for b in range(groups):
            high, low = high_low(rows_b[lanes_of(b), :] * mask_near[lanes_of(a), :])
            right_cat[rows, lanes_of(b)] = high
            right_cat[rows, lanes_of(groups + b)] = high
            right_cat[rows, lanes_of(2 * groups + b)] = low

    def await_first(rows, sem):
        with jax.named_scope("wait_first"):
            await_bytes(have_first, rows, recv_sem, sem)

    def send_mixed_tiles(first, stop, sem):
        with jax.named_scope("send_mixed"):
            send_blocks(first, stop - first, send_mixed, have_mixed, sem, False)

    for a in range(last):
        await_first(2 * groups, a)
        take_left(a)
        take_right(a)
    far_times_near(near_groups, near_groups)
    send_mixed_tiles(0, cut_a, groups + 1)
    await_first(groups, last)
    take_left(last)
    far_times_near([last], near_groups)
    send_mixed_tiles(cut_a, cut_b, groups + 2)
    await_first(groups, groups)
    take_right(last)
    far_times_near(all_groups, [last])
    send_mixed_tiles(cut_b, count, groups + 3)

    sets = ((0, cut_a), (cut_a, cut_b), (cut_b, count))
    for i, (first, stop) in enumerate(sets):
        number = stop - first
        with jax.named_scope("wait_mixed"):
            await_bytes(have_mixed, number, recv_sem, groups + 1 + i)
        values = finish(0, first, number, have_mixed)
        state[:, lanes_of(first, number)] = values
        for t in range(number):
            normalize_into(state[:, lanes_of(first + t)], 1, t, 0)
        side(1, 0, 0, number, send_second, 2 * count, 2 * first)
        if i == 2:
            with jax.named_scope("send_second"):
                send(send_second, have_second, 2 * count, 2 * first, number, groups + 4 + i)
        side(1, 2, 0, number, send_second, 2 * count, 2 * first + number)
        with jax.named_scope("send_second"):
            if i == 2:
                send(send_second, have_second, 2 * count, 2 * first + number, number, groups + 5 + i, "far")
            else:
                send(send_second, have_second, 2 * count, 2 * first, 2 * number, groups + 4 + i)
        gating[:, lanes_of(first, number)] = jax.nn.sigmoid(product(1, 4, 1, 0, number))

    def under_times(firsts, seconds):
        values = jnp.dot(
            left_cat[firsts[0] * span : (firsts[-1] + 1) * span, :],
            under_cat[:, seconds[0] * span : (seconds[-1] + 1) * span],
            preferred_element_type=F32,
        )
        keep_blocks(values, firsts, seconds)

    def take_under_left(first, stop):
        for p in range(first, stop):
            a, b = order[p]
            for b8 in range(half):
                for t, part in enumerate(at_owner(have_second, 2 * count, first + p, b8)):
                    rows_a[pl.ds(t * nr + b8 * SUB, SUB), :] = part
            high, low = high_low((rows_a[0:span, :] * mask_lanes[b, 0:1, :]).T)
            rows = slice(b * span, (b + 1) * span)
            left_cat[rows, lanes_of(a)] = high
            left_cat[rows, lanes_of(groups + a)] = low
            left_cat[rows, lanes_of(2 * groups + a)] = high

    def take_under_right(first, stop):
        for p in range(first, stop):
            a, b = order[p]
            for b8 in range(half):
                for t, part in enumerate(at_owner(have_second, 2 * count, p + stop, b8)):
                    rows_b[pl.ds(t * nr + b8 * SUB, SUB), :] = part
            high, low = high_low(
                rows_b[0:span, :] * mask_lanes[b, 0:1, :] * mask_far[a * span : (a + 1) * span, :]
            )
            under_cat[lanes_of(a), lanes_of(b)] = high
            under_cat[lanes_of(groups + a), lanes_of(b)] = high
            under_cat[lanes_of(2 * groups + a), lanes_of(b)] = low

    def await_second(rows, sem):
        with jax.named_scope("wait_second"):
            await_bytes(have_second, rows, recv_sem, sem)

    def send_next_tiles(first, stop, sem, how):
        with jax.named_scope("send_next"):
            send_blocks(first, stop - first, send_next, have_next, sem, True, how)

    for i in range(2):
        first, stop = sets[i]
        await_second(2 * (stop - first), groups + 4 + i)
        take_under_left(first, stop)
        take_under_right(first, stop)
    under_times(near_groups, near_groups)
    send_next_tiles(0, cut_a, groups + 8, "far")
    await_second(groups, groups + 6)
    take_under_left(cut_b, count)
    under_times([last], near_groups)
    send_next_tiles(cut_a, cut_b, groups + 9, "row")
    await_second(groups, groups + 7)
    take_under_right(cut_b, count)
    under_times(all_groups, [last])
    send_next_tiles(cut_b, count, groups + 10, "row")
    for i, (first, stop) in enumerate(sets):
        with jax.named_scope("wait_next"):
            await_bytes(have_next, stop - first, recv_sem, groups + 8 + i)
        values = finish(1, first, stop - first, have_next)
        for p in range(first, stop):
            tile = values[:, lanes_of(p - first)].T
            for q, rows in enumerate(pieces(p)):
                y_ref[rows, :] = tile[q * SUB : (q + 1) * SUB, :]

    for a in range(last):
        await_bytes(send_first, 2 * groups, send_sem, a)
    for part in range(2):
        await_bytes(send_first, groups, send_sem, last + part)
        await_bytes(send_second, groups, send_sem, groups + 6 + part)
    for i, (first, stop) in enumerate(sets):
        await_bytes(send_mixed, stop - first, send_sem, groups + 1 + i)
        await_bytes(send_next, stop - first, send_sem, groups + 8 + i)
        if i < 2:
            await_bytes(send_second, 2 * (stop - first), send_sem, groups + 4 + i)


def body(
    nr,
    nc,
    pair_state,
    token_mask,
    norm_gain,
    norm_bias,
    proj_weight,
    gate_weight,
    out_gain,
    out_bias,
    out_weight,
):
    ri, cj, channels = pair_state.shape
    hidden = proj_weight.shape[2] // 4
    tokens = token_mask.shape[0]
    slots = nr * nc
    positions = ri * cj
    assert slots == hidden == channels == LANES
    assert nc == SUB and nr == 2 * nc and cj == 2 * ri and tokens == nr * ri == nc * cj
    assert ri % SUB == 0 and ri > SUB and tokens % LANES == 0
    groups = ri // SUB
    count = groups * groups
    message = pltpu.VMEM((slots * count, LANES), F32)
    double = pltpu.VMEM((slots * 2 * count, LANES), F32)
    inputs = (
        pair_state.reshape(positions, channels),
        token_mask.reshape(tokens // LANES, LANES),
        norm_gain,
        norm_bias,
        proj_weight,
        gate_weight,
        out_gain,
        out_bias,
        out_weight,
    )
    result = pl.pallas_call(
        functools.partial(kernel, (nr, nc, ri, cj)),
        out_shape=jax.ShapeDtypeStruct((positions, channels), F32),
        in_specs=[pl.BlockSpec(memory_space=pltpu.HBM)] * len(inputs),
        out_specs=pl.BlockSpec(memory_space=pltpu.VMEM),
        scratch_shapes=[
            *(pltpu.VMEM(i.shape, i.dtype) for i in inputs),
            pltpu.VMEM((2, 6 * LANES, 3 * LANES), BF16),
            pltpu.VMEM((8, LANES, LANES), F32),
            pltpu.VMEM((tokens, LANES), F32),
            pltpu.VMEM((groups, SUB, LANES), F32),
            pltpu.VMEM((tokens, LANES), F32),
            pltpu.VMEM((tokens, LANES), F32),
            pltpu.VMEM((channels, positions), F32),
            pltpu.VMEM((channels, positions), F32),
            pltpu.VMEM((3 * LANES, positions), BF16),
            double,
            double,
            message,
            message,
            double,
            double,
            message,
            message,
            pltpu.VMEM((tokens, LANES), F32),
            pltpu.VMEM((tokens, LANES), F32),
            pltpu.VMEM((tokens, 3 * tokens), BF16),
            pltpu.VMEM((tokens, 3 * tokens), BF16),
            pltpu.VMEM((3 * tokens, tokens), BF16),
            pltpu.VMEM((count * LANES, LANES), F32),
            pltpu.SemaphoreType.DMA((len(inputs),)),
            pltpu.SemaphoreType.DMA((groups + 11,)),
            pltpu.SemaphoreType.DMA((groups + 11,)),
            pltpu.SemaphoreType.REGULAR,
        ],
        compiler_params=pltpu.CompilerParams(
            collective_id=0, has_side_effects=True, vmem_limit_bytes=48 * 2**20
        ),
        name="triangles",
    )(*(pltpu.with_memory_space_constraint(i, pltpu.HBM) for i in inputs))
    return result.reshape(pair_state.shape)


def solution(mesh):
    placed = (P(("groups", "rows"), "cols", None), P("groups"), P(), P(), P(), P(), P(), P(), P())
    return jax.shard_map(
        functools.partial(body, mesh.shape["rows"], mesh.shape["cols"]),
        mesh=mesh,
        in_specs=placed,
        out_specs=P(("groups", "rows"), "cols", None),
        check_vma=False,
    )
```

```python
import functools

import jax
import jax.numpy as jnp
from jax import lax
from jax.experimental import pallas as pl
from jax.experimental.pallas import tpu as pltpu
from jax.sharding import PartitionSpec as P

MESH = pl.DeviceIdType.MESH
eps = 1e-05
LANES = 128
SUB = 8
F32 = jnp.float32
BF16 = jnp.bfloat16


def high_low(values):
    high = values.astype(BF16)
    low = (values - high.astype(F32)).astype(BF16)
    return high, low


def columns_of(row):
    return jnp.broadcast_to(row, (LANES, LANES)).T


def swap_blocks(parts):
    width = LANES // SUB
    block = lax.broadcasted_iota(jnp.int32, (SUB, LANES), 1) // width
    parts = list(parts)
    for step in (1, 2, 4):
        odd = (block // step) % 2 == 1
        for a in range(SUB):
            if (a // step) % 2 == 0:
                low, high = parts[a], parts[a + step]
                parts[a] = jnp.where(odd, pltpu.roll(high, step * width, 1), low)
                parts[a + step] = jnp.where(odd, high, pltpu.roll(low, LANES - step * width, 1))
    return parts


def kernel(
    sizes,
    x_hbm,
    mask_hbm,
    norm_gain_hbm,
    norm_bias_hbm,
    proj_hbm,
    gate_hbm,
    out_gain_hbm,
    out_bias_hbm,
    out_hbm,
    y_ref,
    x_in,
    mask_in,
    norm_gain_in,
    norm_bias_in,
    proj_in,
    gate_in,
    out_gain_in,
    out_bias_in,
    out_in,
    weights,
    columns,
    mask_rows,
    mask_lanes,
    mask_near,
    mask_far,
    state,
    gating,
    normed,
    send_first,
    have_first,
    send_mixed,
    have_mixed,
    send_second,
    have_second,
    send_next,
    have_next,
    rows_a,
    rows_b,
    left_cat,
    right_cat,
    under_cat,
    blocks,
    load_sem,
    send_sem,
    recv_sem,
    ready,
):
    nr, nc, ri, cj = sizes
    slots = nr * nc
    groups = ri // SUB
    half = nr // SUB
    tokens = nr * ri
    span = SUB * nr
    last = groups - 1
    early = [(a, b) for a in range(last) for b in range(last)]
    order = early + [(last, b) for b in range(last)] + [(a, last) for a in range(groups)]
    count = len(order)
    cut_a, cut_b = len(early), len(early) + last
    place = {ab: p for p, ab in enumerate(order)}

    r, c = lax.axis_index("rows"), lax.axis_index("cols")
    me = c * nr + r
    pair, core = r // 2, lax.rem(r, 2)
    pairs = nr // 2
    cols = [lax.rem(c + d, nc) for d in range(nc)]
    cores = [core, 1 - core]
    rows_at = [lax.rem(pair + d, pairs) * 2 for d in range(pairs)]
    turns = [d for d in (4, 1, 7, 2, 6, 3, 5, 0) if d < nc]

    loads = [
        pltpu.make_async_copy(src, dst, load_sem.at[i])
        for i, (src, dst) in enumerate(
            (
                (x_hbm, x_in),
                (norm_gain_hbm, norm_gain_in),
                (norm_bias_hbm, norm_bias_in),
                (proj_hbm, proj_in),
                (mask_hbm, mask_in),
                (gate_hbm, gate_in),
                (out_gain_hbm, out_gain_in),
                (out_bias_hbm, out_bias_in),
                (out_hbm, out_in),
            )
        )
    ]
    for load in loads:
        load.start()

    def to_all(act, how):
        def mixed(i, carry):
            turned = []
            for d in range(pairs):
                far = lax.rem(i + d, pairs)
                turned.append((far, lax.rem(pair + far, pairs) * 2))
            for dx in turns:
                for k in range(2):
                    far, base = turned[(dx + 4 * k) % pairs]
                    row = base + cores[k]

                    def go(row=row, dx=dx):
                        act(cols[dx] * nr + row, {"rows": row, "cols": cols[dx]})

                    if dx == 0 and k == 0:
                        pl.when(far != 0)(go)
                    else:
                        go()
            return carry

        def far_first(i, carry):
            turn, odd = i // 2, lax.rem(i, 2)
            away = pairs // 2 + turn - odd * (2 * turn + 1)
            far_row = lax.rem(pair + away, pairs) * 2
            far_col = lax.rem(c + away, nc)
            for d in turns:
                for k in range(2):
                    row, col = (far_row + cores[0], cols[d]) if k == 0 else (rows_at[d] + cores[1], far_col)

                    def go(row=row, col=col):
                        act(col * nr + row, {"rows": row, "cols": col})

                    if d == 0 and k == 0:
                        pl.when(away != 0)(go)
                    else:
                        go()
            return carry

        def by_row(i, carry):
            for d in sorted(turns, key=lambda d: -min(d, nc - d)):
                for k in range(2):
                    row = i * 2 + cores[k]

                    def go(row=row, d=d):
                        act(cols[d] * nr + row, {"rows": row, "cols": cols[d]})

                    if d == 0 and k == 0:
                        pl.when(i != pair)(go)
                    else:
                        go()
            return carry

        lax.fori_loop(0, pairs, {"mixed": mixed, "far": far_first, "row": by_row}[how], 0)

    barrier = pltpu.get_barrier_semaphore()

    def greet(semaphore):
        to_all(
            lambda slot, device: pl.semaphore_signal(semaphore, inc=1, device_id=device, device_id_type=MESH), "far"
        )

    @pl.when(me != 0)
    def _():
        greet(barrier)

    @pl.when(me == 0)
    def _():
        pl.semaphore_wait(barrier, slots - 1)
        greet(ready)

    def copy_to(src, dst, stride, base, rows, sem):
        def act(slot, device):
            pltpu.make_async_remote_copy(
                src_ref=src.at[pl.ds(slot * stride + base, rows)],
                dst_ref=dst.at[pl.ds(me * stride + base, rows)],
                send_sem=send_sem.at[sem],
                recv_sem=recv_sem.at[sem],
                device_id=device,
                device_id_type=MESH,
            ).start()

        return act

    def keep_own(src, dst, stride, base, rows):
        for q in range(rows):
            dst[pl.ds(me * stride + base + q, 1), :] = src[pl.ds(me * stride + base + q, 1), :]

    def send(src, dst, stride, base, rows, sem, how="mixed"):
        to_all(copy_to(src, dst, stride, base, rows, sem), how)
        keep_own(src, dst, stride, base, rows)

    def await_bytes(buffer, rows, sems, sem):
        whole = buffer.at[pl.ds(0, (slots - 1) * rows)]
        pltpu.make_async_copy(whole, whole, sems.at[sem]).wait()

    def prepare_weights(u):
        def one(values, at):
            high, low = high_low(values.T)
            rows = pl.ds(at * LANES, LANES)
            weights[u, rows, 0:LANES] = high
            weights[u, rows, LANES : 2 * LANES] = low
            weights[u, rows, 2 * LANES : 3 * LANES] = high

        for f in range(4):
            one(proj_in[u, :, f * LANES : (f + 1) * LANES], f)
        one(gate_in[u], 4)
        one(out_in[u], 5)

    def prepare_columns(u):
        for i, ref in enumerate((norm_gain_in, norm_bias_in, out_gain_in, out_bias_in)):
            columns[4 * u + i] = columns_of(ref[pl.ds(u, 1), :])

    def lanes_of(first, number=1):
        return slice(first * LANES, (first + number) * LANES)

    def normalize(values, gain, bias):
        center = values - jnp.mean(values, axis=0, keepdims=True)
        spread = jnp.mean(center * center, axis=0, keepdims=True)
        return center * lax.rsqrt(spread + eps) * gain + bias

    def normalize_into(values, u, at, first):
        high, low = high_low(normalize(values, columns[4 * u + first], columns[4 * u + first + 1]))
        normed[0:LANES, lanes_of(at)] = high
        normed[LANES : 2 * LANES, lanes_of(at)] = high
        normed[2 * LANES : 3 * LANES, lanes_of(at)] = low

    def product(u, first, number, at, tiles):
        return jnp.dot(
            weights[u, first * LANES : (first + number) * LANES, :],
            normed[:, lanes_of(at, tiles)],
            preferred_element_type=F32,
        )

    def side(u, first, at, tiles, buffer, stride, base):
        hidden = product(u, first, 2, at, tiles)
        values = jax.nn.sigmoid(hidden[0:LANES]) * hidden[LANES:]
        for b in range(slots // SUB):
            for t in range(tiles):
                buffer[pl.ds(b * SUB * stride + base + t, SUB, stride=stride), :] = values[
                    b * SUB : (b + 1) * SUB, lanes_of(t)
                ]

    def at_owner(buffer, stride, row, b8):
        return swap_blocks(
            [buffer[pl.ds((a * nr + b8 * SUB) * stride + row, SUB, stride=stride), :] for a in range(nc)]
        )

    def to_owners(parts, buffer, stride, row, b8):
        for a, part in enumerate(swap_blocks(parts)):
            buffer[pl.ds((a * nr + b8 * SUB) * stride + row, SUB, stride=stride), :] = part

    def finish(u, first, number, have):
        for t in range(number):
            normalize_into(
                jnp.concatenate(
                    [have[pl.ds(b * SUB * count + first + t, SUB, stride=count), :] for b in range(slots // SUB)],
                    axis=0,
                ),
                u,
                t,
                2,
            )
        lanes = lanes_of(first, number)
        return state[:, lanes] + gating[:, lanes] * product(u, 5, 1, 0, number)

    def pieces(p):
        a, b = order[p]
        return [
            slice(at, at + SUB)
            for t in range(SUB)
            for parity in range(2)
            for at in ((a * SUB + t) * cj + parity * ri + b * SUB,)
        ]

    for load in loads:
        load.wait()
    prepare_weights(0)
    prepare_columns(0)
    for a in range(groups):
        for b in range(groups):
            p = place[a, b]
            values = jnp.concatenate([x_in[rows, :] for rows in pieces(p)], axis=0).T
            state[:, lanes_of(p)] = values
            normalize_into(values, 0, a * groups + b, 0)
        side(0, 0, a * groups, groups, send_first, 2 * count, 2 * groups * a)
        side(0, 2, a * groups, groups, send_first, 2 * count, 2 * groups * a + groups)
        at = 2 * groups * a
        if a == 0:
            with jax.named_scope("send_first"):
                copy = copy_to(send_first, have_first, 2 * count, at, 2 * groups, a)

                @pl.when(me == 0)
                def _():
                    to_all(copy, "mixed")

                @pl.when(me != 0)
                def _():
                    pl.semaphore_wait(barrier, slots - 2)
                    to_all(lambda slot, device: pl.when(slot != 0)(lambda: copy(slot, device)), "mixed")
                    pl.semaphore_wait(ready, 1)
                    copy(0, {"rows": 0, "cols": 0})

                keep_own(send_first, have_first, 2 * count, at, 2 * groups)
            continue
        with jax.named_scope("send_first"):
            if a < last:
                send(send_first, have_first, 2 * count, at, 2 * groups, a)
            else:
                send(send_first, have_first, 2 * count, at, groups, a)
                send(send_first, have_first, 2 * count, at + groups, groups, a + 1)
    for a in range(groups):
        gate = jax.nn.sigmoid(product(0, 4, 1, a * groups, groups))
        for b in range(groups):
            gating[:, lanes_of(place[a, b])] = gate[:, lanes_of(b)]
    prepare_weights(1)
    prepare_columns(1)
    mask = mask_in[...].astype(F32)
    for t in range(tokens // LANES):
        mask_rows[lanes_of(t), :] = columns_of(mask[t : t + 1, :])
    for a in range(groups):
        near = jnp.concatenate(
            [mask_rows[q * ri + a * SUB : q * ri + (a + 1) * SUB, :] for q in range(nr)], axis=0
        )
        mask_near[lanes_of(a), :] = near
        mask_lanes[a] = near.T[0:SUB, :]
        for t in range(SUB):
            for b8 in range(half):
                mask_far[pl.ds(a * span + t * nr + b8 * SUB, SUB), :] = mask_rows[
                    pl.ds(b8 * SUB * ri + a * SUB + t, SUB, stride=ri), :
                ]

    def send_blocks(first, number, buffer, have, sem, strided, how="mixed"):
        for p in range(first, first + number):
            for b8 in range(half):
                if strided:
                    parts = [blocks[pl.ds(p * span + b8 * SUB * SUB + t, SUB, stride=SUB), :] for t in range(SUB)]
                else:
                    parts = [blocks[pl.ds(p * span + t * nr + b8 * SUB, SUB), :] for t in range(SUB)]
                to_owners(parts, buffer, count, p, b8)
        send(buffer, have, count, first, number, sem, how)

    def keep_blocks(values, firsts, seconds):
        for i, a in enumerate(firsts):
            for j, b in enumerate(seconds):
                blocks[lanes_of(place[a, b]), :] = values[i * span : (i + 1) * span, lanes_of(j)]

    near_groups = list(range(last))
    all_groups = list(range(groups))

    def far_times_near(firsts, seconds):
        values = lax.dot_general(
            left_cat[firsts[0] * span : (firsts[-1] + 1) * span, :],
            right_cat[seconds[0] * span : (seconds[-1] + 1) * span, :],
            (((1,), (1,)), ((), ())),
            preferred_element_type=F32,
        )
        keep_blocks(values, firsts, seconds)

    def take_left(a):
        rows = slice(a * span, (a + 1) * span)
        for b in range(groups):
            for b8 in range(half):
                for t, part in enumerate(at_owner(have_first, 2 * count, 2 * groups * a + b, b8)):
                    rows_a[pl.ds(b * span + t * nr + b8 * SUB, SUB), :] = part
        for b in range(groups):
            high, low = high_low(rows_a[lanes_of(b), :] * mask_lanes[b, 0:1, :] * mask_far[rows, :])
            left_cat[rows, lanes_of(b)] = high
            left_cat[rows, lanes_of(groups + b)] = low
            left_cat[rows, lanes_of(2 * groups + b)] = high

    def take_right(a):
        rows = slice(a * span, (a + 1) * span)
        for b in range(groups):
            for b8 in range(half):
                for t, part in enumerate(at_owner(have_first, 2 * count, 2 * groups * a + groups + b, b8)):
                    rows_b[pl.ds(b * span + b8 * SUB * SUB + t, SUB, stride=SUB), :] = part
        for b in range(groups):
            high, low = high_low(rows_b[lanes_of(b), :] * mask_near[lanes_of(a), :])
            right_cat[rows, lanes_of(b)] = high
            right_cat[rows, lanes_of(groups + b)] = high
            right_cat[rows, lanes_of(2 * groups + b)] = low

    def await_first(rows, sem):
        with jax.named_scope("wait_first"):
            await_bytes(have_first, rows, recv_sem, sem)

    def send_mixed_tiles(first, stop, sem):
        with jax.named_scope("send_mixed"):
            send_blocks(first, stop - first, send_mixed, have_mixed, sem, False)

    for a in range(last):
        await_first(2 * groups, a)
        take_left(a)
        take_right(a)
    far_times_near(near_groups, near_groups)
    send_mixed_tiles(0, cut_a, groups + 1)
    await_first(groups, last)
    take_left(last)
    far_times_near([last], near_groups)
    send_mixed_tiles(cut_a, cut_b, groups + 2)
    await_first(groups, groups)
    take_right(last)
    far_times_near(all_groups, [last])
    send_mixed_tiles(cut_b, count, groups + 3)

    sets = ((0, cut_a), (cut_a, cut_b), (cut_b, count))
    for i, (first, stop) in enumerate(sets):
        number = stop - first
        with jax.named_scope("wait_mixed"):
            await_bytes(have_mixed, number, recv_sem, groups + 1 + i)
        values = finish(0, first, number, have_mixed)
        state[:, lanes_of(first, number)] = values
        for t in range(number):
            normalize_into(state[:, lanes_of(first + t)], 1, t, 0)
        side(1, 0, 0, number, send_second, 2 * count, 2 * first)
        if i == 2:
            with jax.named_scope("send_second"):
                send(send_second, have_second, 2 * count, 2 * first, number, groups + 4 + i, "far")
        side(1, 2, 0, number, send_second, 2 * count, 2 * first + number)
        with jax.named_scope("send_second"):
            if i == 2:
                send(send_second, have_second, 2 * count, 2 * first + number, number, groups + 5 + i, "far")
            else:
                send(send_second, have_second, 2 * count, 2 * first, 2 * number, groups + 4 + i)
        gating[:, lanes_of(first, number)] = jax.nn.sigmoid(product(1, 4, 1, 0, number))

    def under_times(firsts, seconds):
        values = jnp.dot(
            left_cat[firsts[0] * span : (firsts[-1] + 1) * span, :],
            under_cat[:, seconds[0] * span : (seconds[-1] + 1) * span],
            preferred_element_type=F32,
        )
        keep_blocks(values, firsts, seconds)

    def take_under_left(first, stop):
        for p in range(first, stop):
            a, b = order[p]
            for b8 in range(half):
                for t, part in enumerate(at_owner(have_second, 2 * count, first + p, b8)):
                    rows_a[pl.ds(t * nr + b8 * SUB, SUB), :] = part
            high, low = high_low((rows_a[0:span, :] * mask_lanes[b, 0:1, :]).T)
            rows = slice(b * span, (b + 1) * span)
            left_cat[rows, lanes_of(a)] = high
            left_cat[rows, lanes_of(groups + a)] = low
            left_cat[rows, lanes_of(2 * groups + a)] = high

    def take_under_right(first, stop):
        for p in range(first, stop):
            a, b = order[p]
            for b8 in range(half):
                for t, part in enumerate(at_owner(have_second, 2 * count, p + stop, b8)):
                    rows_b[pl.ds(t * nr + b8 * SUB, SUB), :] = part
            high, low = high_low(
                rows_b[0:span, :] * mask_lanes[b, 0:1, :] * mask_far[a * span : (a + 1) * span, :]
            )
            under_cat[lanes_of(a), lanes_of(b)] = high
            under_cat[lanes_of(groups + a), lanes_of(b)] = high
            under_cat[lanes_of(2 * groups + a), lanes_of(b)] = low

    def await_second(rows, sem):
        with jax.named_scope("wait_second"):
            await_bytes(have_second, rows, recv_sem, sem)

    def send_next_tiles(first, stop, sem, how):
        with jax.named_scope("send_next"):
            send_blocks(first, stop - first, send_next, have_next, sem, True, how)

    for i in range(2):
        first, stop = sets[i]
        await_second(2 * (stop - first), groups + 4 + i)
        take_under_left(first, stop)
        take_under_right(first, stop)
    under_times(near_groups, near_groups)
    send_next_tiles(0, cut_a, groups + 8, "far")
    await_second(groups, groups + 6)
    take_under_left(cut_b, count)
    under_times([last], near_groups)
    send_next_tiles(cut_a, cut_b, groups + 9, "row")
    await_second(groups, groups + 7)
    take_under_right(cut_b, count)
    under_times(all_groups, [last])
    send_next_tiles(cut_b, count, groups + 10, "row")
    for i, (first, stop) in enumerate(sets):
        with jax.named_scope("wait_next"):
            await_bytes(have_next, stop - first, recv_sem, groups + 8 + i)
        values = finish(1, first, stop - first, have_next)
        for p in range(first, stop):
            tile = values[:, lanes_of(p - first)].T
            for q, rows in enumerate(pieces(p)):
                y_ref[rows, :] = tile[q * SUB : (q + 1) * SUB, :]

    for a in range(last):
        await_bytes(send_first, 2 * groups, send_sem, a)
    for part in range(2):
        await_bytes(send_first, groups, send_sem, last + part)
        await_bytes(send_second, groups, send_sem, groups + 6 + part)
    for i, (first, stop) in enumerate(sets):
        await_bytes(send_mixed, stop - first, send_sem, groups + 1 + i)
        await_bytes(send_next, stop - first, send_sem, groups + 8 + i)
        if i < 2:
            await_bytes(send_second, 2 * (stop - first), send_sem, groups + 4 + i)


def body(
    nr,
    nc,
    pair_state,
    token_mask,
    norm_gain,
    norm_bias,
    proj_weight,
    gate_weight,
    out_gain,
    out_bias,
    out_weight,
):
    ri, cj, channels = pair_state.shape
    hidden = proj_weight.shape[2] // 4
    tokens = token_mask.shape[0]
    slots = nr * nc
    positions = ri * cj
    assert slots == hidden == channels == LANES
    assert nc == SUB and nr == 2 * nc and cj == 2 * ri and tokens == nr * ri == nc * cj
    assert ri % SUB == 0 and ri > SUB and tokens % LANES == 0
    groups = ri // SUB
    count = groups * groups
    message = pltpu.VMEM((slots * count, LANES), F32)
    double = pltpu.VMEM((slots * 2 * count, LANES), F32)
    inputs = (
        pair_state.reshape(positions, channels),
        token_mask.reshape(tokens // LANES, LANES),
        norm_gain,
        norm_bias,
        proj_weight,
        gate_weight,
        out_gain,
        out_bias,
        out_weight,
    )
    result = pl.pallas_call(
        functools.partial(kernel, (nr, nc, ri, cj)),
        out_shape=jax.ShapeDtypeStruct((positions, channels), F32),
        in_specs=[pl.BlockSpec(memory_space=pltpu.HBM)] * len(inputs),
        out_specs=pl.BlockSpec(memory_space=pltpu.VMEM),
        scratch_shapes=[
            *(pltpu.VMEM(i.shape, i.dtype) for i in inputs),
            pltpu.VMEM((2, 6 * LANES, 3 * LANES), BF16),
            pltpu.VMEM((8, LANES, LANES), F32),
            pltpu.VMEM((tokens, LANES), F32),
            pltpu.VMEM((groups, SUB, LANES), F32),
            pltpu.VMEM((tokens, LANES), F32),
            pltpu.VMEM((tokens, LANES), F32),
            pltpu.VMEM((channels, positions), F32),
            pltpu.VMEM((channels, positions), F32),
            pltpu.VMEM((3 * LANES, positions), BF16),
            double,
            double,
            message,
            message,
            double,
            double,
            message,
            message,
            pltpu.VMEM((tokens, LANES), F32),
            pltpu.VMEM((tokens, LANES), F32),
            pltpu.VMEM((tokens, 3 * tokens), BF16),
            pltpu.VMEM((tokens, 3 * tokens), BF16),
            pltpu.VMEM((3 * tokens, tokens), BF16),
            pltpu.VMEM((count * LANES, LANES), F32),
            pltpu.SemaphoreType.DMA((len(inputs),)),
            pltpu.SemaphoreType.DMA((groups + 11,)),
            pltpu.SemaphoreType.DMA((groups + 11,)),
            pltpu.SemaphoreType.REGULAR,
        ],
        compiler_params=pltpu.CompilerParams(
            collective_id=0, has_side_effects=True, vmem_limit_bytes=48 * 2**20
        ),
        name="triangles",
    )(*(pltpu.with_memory_space_constraint(i, pltpu.HBM) for i in inputs))
    return result.reshape(pair_state.shape)


def solution(mesh):
    placed = (P(("groups", "rows"), "cols", None), P("groups"), P(), P(), P(), P(), P(), P(), P())
    return jax.shard_map(
        functools.partial(body, mesh.shape["rows"], mesh.shape["cols"]),
        mesh=mesh,
        in_specs=placed,
        out_specs=P(("groups", "rows"), "cols", None),
        check_vma=False,
    )
```
